32 devices in a mesh: dp: 2 (over x), sw: 4 (over z), sh: 4 (over y, core).
Axes of the slice: x: 2, y: 2, z: 4, core: 2. Of those that a mesh axis runs over, the one named last changes fastest.
Arguments:
- feat_map: bfloat16 [24, 384, 64, 80], P('dp', 'sh', 'sw'), parts along dimension 0
- norm0_w: bfloat16 [80], replicated
- norm0_b: bfloat16 [80], replicated
- down_w: bfloat16 [2, 2, 80, 160], replicated
- down_b: bfloat16 [160], replicated
- dw_w: bfloat16 [2, 7, 7, 160], replicated
- dw_b: bfloat16 [2, 160], replicated
- norm_w: bfloat16 [2, 160], replicated
- norm_b: bfloat16 [2, 160], replicated
- pw1_w: bfloat16 [2, 160, 640], replicated
- pw1_b: bfloat16 [2, 640], replicated
- pw2_w: bfloat16 [2, 640, 160], replicated
- pw2_b: bfloat16 [2, 160], replicated
- layer_scale: bfloat16 [2, 160], replicated
Outputs:
- output: bfloat16 [24, 192, 32, 160], P('dp', 'sh', 'sw'), parts along dimension 0
There are 2 independent parts. The reference program is written for one: setup_inputs(seed, part) draws one part's arguments, and reference() takes and returns one part's arrays. A program takes and returns all parts, laid end to end along the dimension named above; an argument that names none is the same for every part.
All inputs are finite; a program needn't handle non-finite values.
Results may differ from the reference program's by a relative error of at most 0.0119833.
Values are sent between devices in bfloat16 or wider.
A program may use at most 1 GiB of HBM per device.

```python
import jax
import jax.numpy as jnp
from jax import lax

BATCH = 12
IMG_H = 384
IMG_W = 64
CH_IN = 80
CH_OUT = 160

LN_EPS = 1e-6
CONV_DIMS = ("NHWC", "HWIO", "NHWC")


def layer_norm(values, gain_vec, shift_vec):
    mean_val = jnp.mean(values, axis=-1, keepdims=True)
    centered = values - mean_val
    var_val = jnp.mean(centered * centered, axis=-1, keepdims=True)
    return centered * lax.rsqrt(var_val + LN_EPS) * gain_vec.astype(jnp.float32) + shift_vec.astype(jnp.float32)


def setup_inputs(seed: int = 0, part: int = 0) -> dict:
    keys = jax.random.split(jax.random.key(seed), 16)
    img_key = jax.random.fold_in(keys[0], part)
    coarse_key, fine_key = jax.random.split(img_key)
    coarse = jax.random.normal(coarse_key, (BATCH, IMG_H // 8, IMG_W // 8, CH_IN), jnp.float32)
    coarse = jnp.repeat(jnp.repeat(coarse, 8, axis=1), 8, axis=2)
    fine = jax.random.normal(fine_key, (BATCH, IMG_H, IMG_W, CH_IN), jnp.float32)
    hidden = 4 * CH_OUT

    def normal(key_index, array_shape, spread):
        return spread * jax.random.normal(keys[key_index], array_shape, jnp.float32)

    return {
        "feat_map": (coarse + 0.5 * fine).astype(jnp.bfloat16),
        "norm0_w": (1.0 + normal(1, (CH_IN,), 0.3)).astype(jnp.bfloat16),
        "norm0_b": normal(2, (CH_IN,), 0.3).astype(jnp.bfloat16),
        "down_w": normal(3, (2, 2, CH_IN, CH_OUT), (4 * CH_IN) ** -0.5).astype(jnp.bfloat16),
        "down_b": normal(4, (CH_OUT,), 0.3).astype(jnp.bfloat16),
        "dw_w": normal(5, (2, 7, 7, CH_OUT), 1.0 / 7.0).astype(jnp.bfloat16),
        "dw_b": normal(6, (2, CH_OUT), 0.5).astype(jnp.bfloat16),
        "norm_w": (1.0 + normal(7, (2, CH_OUT), 0.3)).astype(jnp.bfloat16),
        "norm_b": normal(8, (2, CH_OUT), 0.3).astype(jnp.bfloat16),
        "pw1_w": normal(9, (2, CH_OUT, hidden), CH_OUT ** -0.5).astype(jnp.bfloat16),
        "pw1_b": normal(10, (2, hidden), 0.3).astype(jnp.bfloat16),
        "pw2_w": normal(11, (2, hidden, CH_OUT), hidden ** -0.5).astype(jnp.bfloat16),
        "pw2_b": normal(12, (2, CH_OUT), 0.3).astype(jnp.bfloat16),
        "layer_scale": jax.random.uniform(keys[13], (2, CH_OUT), jnp.float32, 0.2, 1.0).astype(jnp.bfloat16),
    }


def reference(feat_map, norm0_w, norm0_b, down_w, down_b, dw_w, dw_b, norm_w, norm_b, pw1_w, pw1_b, pw2_w, pw2_b, layer_scale):
    block_params = (dw_w, dw_b, norm_w, norm_b, pw1_w, pw1_b, pw2_w, pw2_b, layer_scale)

    def one_image(image):
        normed = layer_norm(image.astype(jnp.float32), norm0_w, norm0_b).astype(jnp.bfloat16)
        reduced = lax.conv_general_dilated(normed[None].astype(jnp.float32), down_w.astype(jnp.float32), (2, 2), "VALID", dimension_numbers=CONV_DIMS)[0]
        state = (reduced + down_b.astype(jnp.float32)).astype(jnp.bfloat16)

        def one_block(carry, weights):
            w_dw, b_dw, w_norm, b_norm, w_up, b_up, w_down, b_down, scale_vec = weights
            mixed = lax.conv_general_dilated(carry[None].astype(jnp.float32), w_dw[:, :, None, :].astype(jnp.float32), (1, 1), [(3, 3), (3, 3)], dimension_numbers=CONV_DIMS, feature_group_count=CH_OUT)[0]
            mixed = mixed + b_dw.astype(jnp.float32)

            def one_row(pair):
                mixed_row, carry_row = pair
                normed_row = layer_norm(mixed_row, w_norm, b_norm).astype(jnp.bfloat16)
                hidden_row = jnp.dot(normed_row, w_up, preferred_element_type=jnp.float32) + b_up.astype(jnp.float32)
                hidden_row = jax.nn.gelu(hidden_row, approximate=False).astype(jnp.bfloat16)
                proj_row = jnp.dot(hidden_row, w_down, preferred_element_type=jnp.float32) + b_down.astype(jnp.float32)
                return (carry_row.astype(jnp.float32) + scale_vec.astype(jnp.float32) * proj_row).astype(jnp.bfloat16)

            return lax.map(one_row, (mixed, carry)), None

        return lax.scan(one_block, state, block_params)[0]

    return lax.map(one_image, feat_map)
```

```python
import functools

import jax
import jax.numpy as jnp
from jax import lax
from jax.experimental import pallas as pl
from jax.experimental.pallas import tpu as pltpu
from jax.sharding import PartitionSpec as P

LN_EPS = 1e-6
MESH = pl.DeviceIdType.MESH
GI = 4
NPL = GI + 1
LANES = 128
TAIL = 32
ROW = 24
COL0 = 8
BORDER = 3
HALF = 0.5
RSQRT2X2 = 1.4142135623730951

F32 = jnp.float32
BF16 = jnp.bfloat16


def kernel(
    rows_count, cols_count,
    feat, norm0_w, norm0_b, down_w, down_b, dw_w, dw_b, norm_w, norm_b, pw1_w, pw1_b, pw2_w, pw2_b, layer_scale,
    out,
    fv, s0, s1, pad, hsend, hrecv, csend, crecv, cstage, ubuf, vbuf, ybuf, wd, w1, w2, dwf, vec, obuf,
    feat_sem, out_sem, send_sem, recv_sem,
):
    images, _, _, ch_in = fv.shape
    groups = images // GI
    tile_h, tile_w = obuf.shape[1], obuf.shape[2]
    pix = tile_h * tile_w
    my_row, my_col = lax.axis_index("sh"), lax.axis_index("sw")
    has_up, has_down = my_row > 0, my_row < rows_count - 1
    has_left, has_right = my_col > 0, my_col < cols_count - 1

    steps = [(-1, 0), (1, 0), (0, -1), (0, 1), (-1, -1), (-1, 1), (1, -1), (1, 1)]
    row_ok = {-1: has_up, 0: None, 1: has_down}
    col_ok = {-1: has_left, 0: None, 1: has_right}

    def exists(q):
        dr, dc = steps[q]
        if row_ok[dr] is None:
            return col_ok[dc]
        if col_ok[dc] is None:
            return row_ok[dr]
        return jnp.logical_and(row_ok[dr], col_ok[dc])

    def opposite(q):
        dr, dc = steps[q]
        return steps.index((-dr, -dc))

    def device(q):
        dr, dc = steps[q]
        return {"sh": my_row + dr, "sw": my_col + dc}

    feat_copies = [pltpu.make_async_copy(feat.at[i], fv.at[i], feat_sem.at[i]) for i in range(images)]
    for copy in feat_copies:
        copy.start()

    barrier = pltpu.get_barrier_semaphore()
    for q in range(8):
        @pl.when(exists(q))
        def _():
            pl.semaphore_signal(barrier, inc=1, device_id=device(q), device_id_type=MESH)

    def zero_rows(first):
        def body(p, _):
            pad[p, pl.ds(first, BORDER)] = jnp.zeros((BORDER, ROW, LANES), F32)
            return 0
        lax.fori_loop(0, pad.shape[0], body, 0)

    def zero_cols(first):
        def body(p, _):
            pad[p, :, pl.ds(first, 8)] = jnp.zeros((pad.shape[1], 8, LANES), F32)
            return 0
        lax.fori_loop(0, pad.shape[0], body, 0)

    pl.when(jnp.logical_not(has_up))(lambda: zero_rows(0))
    pl.when(jnp.logical_not(has_down))(lambda: zero_rows(BORDER + tile_h))
    pl.when(jnp.logical_not(has_left))(lambda: zero_cols(0))
    pl.when(jnp.logical_not(has_right))(lambda: zero_cols(COL0 + tile_w))

    s0[...] = jnp.zeros(s0.shape, F32)
    s1[...] = jnp.zeros(s1.shape, F32)

    def tail_at(tail, slot):
        rows = tail.shape[0]
        parts = [tail]
        if slot:
            parts = [jnp.zeros((rows, TAIL * slot), tail.dtype)] + parts
        if slot < GI - 1:
            parts = parts + [jnp.zeros((rows, TAIL * (GI - 1 - slot)), tail.dtype)]
        return jnp.concatenate(parts, axis=1)

    for tap in range(4):
        taps = down_w[tap // 2, tap % 2].astype(F32)
        zeros = jnp.zeros((LANES - ch_in, 2 * LANES), BF16)
        for slot in range(GI):
            wd[slot, pl.ds(tap * LANES, ch_in), :LANES] = taps[:, :LANES].astype(BF16)
            wd[slot, pl.ds(tap * LANES, ch_in), LANES:] = tail_at(taps[:, LANES:], slot).astype(BF16)
            wd[slot, pl.ds(tap * LANES + ch_in, LANES - ch_in)] = zeros
    for k in range(2):
        for slot in range(GI):
            w1[k, slot, :LANES] = (pw1_w[k, :LANES, :].astype(F32) * HALF).astype(BF16)
            w1[k, slot, LANES:] = jnp.zeros((LANES, w1.shape[3]), BF16)
            w1[k, slot, pl.ds(LANES + TAIL * slot, TAIL)] = (pw1_w[k, LANES:, :].astype(F32) * HALF).astype(BF16)
            w2[k, slot, :, :LANES] = pw2_w[k, :, :LANES]
            w2[k, slot, :, LANES:] = tail_at(pw2_w[k, :, LANES:].astype(F32), slot).astype(BF16)
        for kh in range(7):
            taps = dw_w[k, kh].astype(F32)
            dwf[k, 0, kh, :7] = taps[:, :LANES]
            dwf[k, 1, kh, :7] = jnp.concatenate([taps[:, LANES:]] * GI, axis=1)

    def split(row):
        row = row.astype(F32)
        return row[:, :LANES], jnp.concatenate([row[:, LANES:]] * GI, axis=1)

    names = [dw_b, norm_w, norm_b, pw2_b, layer_scale]
    for k in range(2):
        for j, ref in enumerate(names):
            head, tail = split(ref[k:k + 1, :])
            vec[k, 0, j:j + 1] = head
            vec[k, 1, j:j + 1] = tail
    head, tail = split(down_b[...])
    vec[0, 0, 5:6] = head
    vec[0, 1, 5:6] = tail

    flat = pad.reshape(pad.shape[0], pad.shape[1] * ROW, LANES)

    def column(plane, row, col, count):
        return flat.at[plane, pl.ds((BORDER + row) * ROW + COL0 + col, count, stride=ROW), :]

    def messages(k, g):
        base = k * groups * NPL + g * NPL
        planes = pl.ds(base, NPL)
        copies = []
        for q, (dr, dc) in enumerate(steps):
            there = opposite(q)
            if dc == 0:
                first = BORDER if dr < 0 else tile_h
                land = BORDER + tile_h if dr < 0 else 0
                src = pad.at[planes, pl.ds(first, BORDER), pl.ds(COL0, tile_w), :]
                dst = pad.at[planes, pl.ds(land, BORDER), pl.ds(COL0, tile_w), :]
            elif dr == 0:
                src = hsend.at[k, g, q - 2]
                dst = hrecv.at[k, g, there - 2]
            else:
                src = csend.at[k, g, q - 4]
                dst = crecv.at[k, g, there - 4]
            copies.append(pltpu.make_async_remote_copy(
                src_ref=src, dst_ref=dst, send_sem=send_sem.at[k, g, q], recv_sem=recv_sem.at[k, g, there],
                device_id=device(q), device_id_type=MESH))
        return copies

    def send(k, g):
        base = k * groups * NPL + g * NPL
        copies = messages(k, g)
        for q in (2, 3):
            first = 0 if q == 2 else tile_w - BORDER

            def fill(p, _):
                for j in range(BORDER):
                    hsend[k, g, q - 2, p * BORDER + j] = column(base + p, 0, first + j, tile_h)[...].astype(BF16)
                return 0

            lax.fori_loop(0, NPL, fill, 0)
        for q in range(4, 8):
            dr, dc = steps[q]
            first = 0 if dc < 0 else tile_w - BORDER
            row = 0 if dr < 0 else tile_h - BORDER
            for p in range(NPL):
                for j in range(BORDER):
                    cstage[pl.ds((p * BORDER + j) * BORDER, BORDER)] = column(base + p, row, first + j, BORDER)[...]
            csend[k, g, q - 4] = cstage[...].astype(BF16)
        for q in range(8):
            pl.when(exists(q))(copies[q].start)

    def receive(k, g):
        base = k * groups * NPL + g * NPL
        copies = messages(k, g)
        for q in range(8):
            pl.when(exists(q))(_wait_recv(k, g, q))
        for q in (2, 3):
            first = -BORDER if q == 2 else tile_w

            @pl.when(exists(q))
            def _():
                def put(p, _):
                    for j in range(BORDER):
                        column(base + p, 0, first + j, tile_h)[...] = hrecv[k, g, q - 2, p * BORDER + j].astype(F32)
                    return 0

                lax.fori_loop(0, NPL, put, 0)
        for q in range(4, 8):
            dr, dc = steps[q]
            first = -BORDER if dc < 0 else tile_w
            row = -BORDER if dr < 0 else tile_h

            @pl.when(exists(q))
            def _():
                cstage[...] = crecv[k, g, q - 4].astype(F32)
                for p in range(NPL):
                    for j in range(BORDER):
                        column(base + p, row, first + j, BORDER)[...] = cstage[pl.ds((p * BORDER + j) * BORDER, BORDER)]

    def _wait_recv(k, g, q):
        base = k * groups * NPL + g * NPL
        dr, dc = steps[q]
        if dc == 0:
            land = 0 if dr < 0 else BORDER + tile_h
            dst = pad.at[pl.ds(base, NPL), pl.ds(land, BORDER), pl.ds(COL0, tile_w), :]
        elif dr == 0:
            dst = hrecv.at[k, g, q - 2]
        else:
            dst = crecv.at[k, g, q - 4]

        def wait():
            pltpu.make_async_remote_copy(
                src_ref=dst, dst_ref=dst, send_sem=send_sem.at[k, g, q], recv_sem=recv_sem.at[k, g, q],
                device_id=device(q), device_id_type=MESH).wait_recv()

        return wait

    def wait_send(k, g):
        copies = messages(k, g)
        for q in range(8):
            pl.when(exists(q))(copies[q].wait_send)

    def interior(plane):
        return pad.at[plane, pl.ds(BORDER, tile_h), pl.ds(COL0, tile_w), :]

    def rounded(values):
        return values.astype(BF16).astype(F32)

    w0 = norm0_w[...].astype(F32)
    b0 = norm0_b[...].astype(F32)

    def down_image(g, i):
        img = g * GI + i
        pltpu.make_async_copy(feat.at[img], fv.at[img], feat_sem.at[img]).wait()
        for kh, stage in ((0, s0), (1, s1)):
            x = fv[img].astype(F32).reshape(tile_h, 2, 2 * tile_w, ch_in)[:, kh].reshape(tile_h * 2 * tile_w, ch_in)
            mean = jnp.sum(x, axis=-1, keepdims=True) * (1.0 / ch_in)
            centered = x - mean
            var = jnp.sum(centered * centered, axis=-1, keepdims=True) * (1.0 / ch_in)
            stage[:, :ch_in] = centered * lax.rsqrt(var + LN_EPS) * w0 + b0
        taps = [s[pl.ds(kw, pix, stride=2), :].astype(BF16) for s in (s0, s1) for kw in (0, 1)]
        d = jnp.dot(jnp.concatenate(taps, axis=1), wd[i], preferred_element_type=F32)
        head = rounded(d[:, :LANES] + vec[0, 0, 5:6])
        interior(g * NPL + i)[...] = head.reshape(tile_h, tile_w, LANES)
        return d[:, LANES:]

    def down_group(g, _):
        ybuf[...] = jnp.zeros(ybuf.shape, F32)

        def one(i, _):
            ybuf[...] += down_image(g, i)
            return 0

        lax.fori_loop(0, GI, one, 0)
        tail = rounded(ybuf[...] + vec[0, 1, 5:6])
        interior(g * NPL + GI)[...] = tail.reshape(tile_h, tile_w, LANES)

        @pl.when(g == 0)
        def _():
            count = jnp.int32(0)
            for q in range(8):
                count = count + exists(q).astype(jnp.int32)
            pl.semaphore_wait(barrier, count)

        send(0, g)
        return 0

    R = 16
    strips = tile_h // R

    def depthwise(k, g):
        base = k * groups * NPL + g * NPL

        def body(t, _):
            p, strip = t // strips, t % strips
            part = (p == GI).astype(jnp.int32)
            r0 = strip * R
            accs = [None] * R
            bias = vec[k, part, 0:1]
            for kw in range(7):
                xs = [pad[base + p, r0 + i, COL0 - BORDER + kw:COL0 - BORDER + kw + 8, :] for i in range(R + 6)]
                for kh in range(7):
                    w = jnp.broadcast_to(dwf[k, part, kh, kw:kw + 1, :], (8, LANES))
                    for r in range(R):
                        term = xs[r + kh] * w
                        accs[r] = term if accs[r] is None else accs[r] + term
            for r in range(R):
                ubuf[p, pl.ds((r0 + r) * 8, 8)] = accs[r] + bias
            return 0

        lax.fori_loop(0, NPL * strips, body, 0)

    LR = 64

    def norm(k):
        nw, nb = vec[k, 0, 1:2], vec[k, 0, 2:3]
        nwt, nbt = vec[k, 1, 1:2], vec[k, 1, 2:3]
        lane = lax.broadcasted_iota(jnp.int32, (LR, LANES), 1)
        channels = LANES + TAIL

        def body(t, _):
            rows = pl.ds(pl.multiple_of(t * LR, LR), LR)
            tail = ubuf[GI, rows]
            heads = [ubuf[i, rows] for i in range(GI)]
            own = [jnp.logical_and(lane >= i * TAIL, lane < (i + 1) * TAIL) for i in range(GI)]

            def pick(cols):
                res = cols[GI - 1]
                for i in range(GI - 2, -1, -1):
                    res = jnp.where(lane < (i + 1) * TAIL, cols[i], res)
                return res

            means = [jnp.sum(heads[i] + jnp.where(own[i], tail, 0.0), axis=-1, keepdims=True) * (1.0 / channels) for i in range(GI)]
            heads = [heads[i] - means[i] for i in range(GI)]
            tail = tail - pick(means)
            square = tail * tail
            rs = [lax.rsqrt(jnp.sum(heads[i] * heads[i] + jnp.where(own[i], square, 0.0), axis=-1, keepdims=True) * (1.0 / channels) + LN_EPS) for i in range(GI)]
            for i in range(GI):
                vbuf[i, rows] = (heads[i] * rs[i] * nw + nb).astype(BF16)
            vbuf[GI, rows] = (tail * pick(rs) * nwt + nbt).astype(BF16)
            return 0

        lax.fori_loop(0, pix // LR, body, 0)

    def mlp(k, g):
        base = k * groups * NPL + g * NPL
        nxt = groups * NPL + g * NPL
        b1 = pw1_b[k:k + 1, :].astype(F32) * HALF
        ybuf[...] = jnp.zeros(ybuf.shape, F32)

        def body(i, _):
            v = jnp.concatenate([vbuf[i], vbuf[GI]], axis=1)
            x = jnp.dot(v, w1[k, i], preferred_element_type=F32) + b1
            hidden = (x + x * lax.erf(x * RSQRT2X2)).astype(BF16)
            y = jnp.dot(hidden, w2[k, i], preferred_element_type=F32)
            head = (y[:, :LANES] + vec[k, 0, 3:4]) * vec[k, 0, 4:5]
            ybuf[...] += y[:, LANES:]
            new = interior(base + i)[...] + head.reshape(tile_h, tile_w, LANES)
            if k == 0:
                interior(nxt + i)[...] = rounded(new)
            else:
                obuf[g * GI + i, :, :, :LANES] = new.astype(BF16)
            return 0

        lax.fori_loop(0, GI, body, 0)
        tail = ((ybuf[...] + vec[k, 1, 3:4]) * vec[k, 1, 4:5]).reshape(tile_h, tile_w, LANES)
        new = interior(base + GI)[...] + tail
        if k == 0:
            interior(nxt + GI)[...] = rounded(new)
        else:
            for i in range(GI):
                obuf[g * GI + i, :, :, LANES:] = new[:, :, i * TAIL:(i + 1) * TAIL].astype(BF16)

    def out_copy(g):
        imgs = pl.ds(g * GI, GI)
        return pltpu.make_async_copy(obuf.at[imgs], out.at[imgs], out_sem.at[g])

    def block_group(k):
        def body(g, _):
            receive(k, g)
            depthwise(k, g)
            norm(k)
            mlp(k, g)
            if k == 0:
                send(1, g)
            else:
                out_copy(g).start()
            return 0
        return body

    lax.fori_loop(0, groups, down_group, 0)
    lax.fori_loop(0, groups, block_group(0), 0)
    lax.fori_loop(0, groups, block_group(1), 0)

    def finish(g, _):
        wait_send(0, g)
        wait_send(1, g)
        out_copy(g).wait()
        return 0

    lax.fori_loop(0, groups, finish, 0)


def solution(mesh):
    rows_count = mesh.shape["sh"]
    cols_count = mesh.shape["sw"]
    act_spec = P("dp", "sh", "sw", None)

    def local_run(feat_map, norm0_w, norm0_b, down_w, down_b, dw_w, dw_b, norm_w, norm_b, pw1_w, pw1_b, pw2_w, pw2_b, layer_scale):
        images, in_h, in_w, ch_in = feat_map.shape
        tile_h, tile_w = in_h // 2, in_w // 2
        ch, hidden = pw1_w.shape[1:]
        groups = images // GI
        pix = tile_h * tile_w
        vmem = pl.BlockSpec(memory_space=pltpu.VMEM)
        hbm = pl.BlockSpec(memory_space=pl.ANY)
        return pl.pallas_call(
            functools.partial(kernel, rows_count, cols_count),
            out_shape=jax.ShapeDtypeStruct((images, tile_h, tile_w, ch), BF16),
            in_specs=[hbm] + [vmem] * 13,
            out_specs=hbm,
            scratch_shapes=[
                pltpu.VMEM((images, in_h, in_w, ch_in), BF16),
                pltpu.VMEM((2 * pix, LANES), F32),
                pltpu.VMEM((2 * pix, LANES), F32),
                pltpu.VMEM((2 * groups * NPL, tile_h + 2 * BORDER, ROW, LANES), F32),
                pltpu.VMEM((2, groups, 2, NPL * BORDER, tile_h, LANES), BF16),
                pltpu.VMEM((2, groups, 2, NPL * BORDER, tile_h, LANES), BF16),
                pltpu.VMEM((2, groups, 4, 48, LANES), BF16),
                pltpu.VMEM((2, groups, 4, 48, LANES), BF16),
                pltpu.VMEM((48, LANES), F32),
                pltpu.VMEM((NPL, pix, LANES), F32),
                pltpu.VMEM((NPL, pix, LANES), BF16),
                pltpu.VMEM((pix, LANES), F32),
                pltpu.VMEM((GI, 4 * LANES, 2 * LANES), BF16),
                pltpu.VMEM((2, GI, 2 * LANES, hidden), BF16),
                pltpu.VMEM((2, GI, hidden, 2 * LANES), BF16),
                pltpu.VMEM((2, 2, 7, 8, LANES), F32),
                pltpu.VMEM((2, 2, 8, LANES), F32),
                pltpu.VMEM((images, tile_h, tile_w, ch), BF16),
                pltpu.SemaphoreType.DMA((images,)),
                pltpu.SemaphoreType.DMA((groups,)),
                pltpu.SemaphoreType.DMA((2, groups, 8)),
                pltpu.SemaphoreType.DMA((2, groups, 8)),
            ],
            compiler_params=pltpu.CompilerParams(collective_id=0, has_side_effects=True, vmem_limit_bytes=63 * 1024 * 1024),
        )(feat_map, norm0_w.reshape(1, -1), norm0_b.reshape(1, -1), down_w, down_b.reshape(1, -1), dw_w, dw_b, norm_w, norm_b, pw1_w, pw1_b, pw2_w, pw2_b, layer_scale)

    return jax.shard_map(local_run, mesh=mesh, in_specs=(act_spec,) + (P(),) * 13, out_specs=act_spec, check_vma=False)
```

```python
import functools

import jax
import jax.numpy as jnp
from jax import lax
from jax.experimental import pallas as pl
from jax.experimental.pallas import tpu as pltpu
from jax.sharding import PartitionSpec as P

LN_EPS = 1e-6
MESH = pl.DeviceIdType.MESH
GI = 4
NPL = GI + 1
LANES = 128
TAIL = 32
ROW = 24
COL0 = 8
BORDER = 3
HALF = 0.5
RSQRT2X2 = 1.4142135623730951

F32 = jnp.float32
BF16 = jnp.bfloat16


def kernel(
    rows_count, cols_count,
    feat, norm0_w, norm0_b, down_w, down_b, dw_w, dw_b, norm_w, norm_b, pw1_w, pw1_b, pw2_w, pw2_b, layer_scale,
    out,
    fv, ab, sel, norm0, pad, hsend, hrecv, csend, crecv, cstage, ubuf, vbuf, ybuf, wd, w1, w2, dwf, vec, obuf,
    feat_sem, out_sem, send_sem, recv_sem,
):
    images, in_w, ch_in, in_h = fv.shape
    groups = images // GI
    tile_h, tile_w = obuf.shape[1], obuf.shape[2]
    pix = tile_h * tile_w
    my_row, my_col = lax.axis_index("sh"), lax.axis_index("sw")
    has_up, has_down = my_row > 0, my_row < rows_count - 1
    has_left, has_right = my_col > 0, my_col < cols_count - 1

    steps = [(-1, 0), (1, 0), (0, -1), (0, 1), (-1, -1), (-1, 1), (1, -1), (1, 1)]
    row_ok = {-1: has_up, 0: None, 1: has_down}
    col_ok = {-1: has_left, 0: None, 1: has_right}

    def exists(q):
        dr, dc = steps[q]
        if row_ok[dr] is None:
            return col_ok[dc]
        if col_ok[dc] is None:
            return row_ok[dr]
        return jnp.logical_and(row_ok[dr], col_ok[dc])

    def opposite(q):
        dr, dc = steps[q]
        return steps.index((-dr, -dc))

    def device(q):
        dr, dc = steps[q]
        return {"sh": my_row + dr, "sw": my_col + dc}

    feat_copies = [pltpu.make_async_copy(feat.at[i], fv.at[i], feat_sem.at[i]) for i in range(images)]
    for copy in feat_copies:
        copy.start()

    barrier = pltpu.get_barrier_semaphore()
    for q in range(8):
        @pl.when(exists(q))
        def _():
            pl.semaphore_signal(barrier, inc=1, device_id=device(q), device_id_type=MESH)

    def zero_rows(first):
        def body(p, _):
            pad[p, pl.ds(first, BORDER)] = jnp.zeros((BORDER, ROW, LANES), F32)
            return 0
        lax.fori_loop(0, pad.shape[0], body, 0)

    def zero_cols(first):
        def body(p, _):
            pad[p, :, pl.ds(first, 8)] = jnp.zeros((pad.shape[1], 8, LANES), F32)
            return 0
        lax.fori_loop(0, pad.shape[0], body, 0)

    pl.when(jnp.logical_not(has_up))(lambda: zero_rows(0))
    pl.when(jnp.logical_not(has_down))(lambda: zero_rows(BORDER + tile_h))
    pl.when(jnp.logical_not(has_left))(lambda: zero_cols(0))
    pl.when(jnp.logical_not(has_right))(lambda: zero_cols(COL0 + tile_w))

    ab[...] = jnp.zeros(ab.shape, BF16)
    row_id = lax.broadcasted_iota(jnp.int32, sel.shape, 0)
    col_id = lax.broadcasted_iota(jnp.int32, sel.shape, 1)
    picked = jnp.where(row_id < tile_h, 2 * row_id, 2 * (row_id - tile_h) + 1)
    sel[...] = jnp.where(col_id == picked, 1.0, 0.0).astype(BF16)
    norm0[0] = jnp.broadcast_to(norm0_w[...].astype(F32), (LANES, ch_in)).T
    norm0[1] = jnp.broadcast_to(norm0_b[...].astype(F32), (LANES, ch_in)).T
    cstage[...] = jnp.zeros(cstage.shape, F32)

    def tail_at(tail, slot):
        rows = tail.shape[0]
        parts = [tail]
        if slot:
            parts = [jnp.zeros((rows, TAIL * slot), tail.dtype)] + parts
        if slot < GI - 1:
            parts = parts + [jnp.zeros((rows, TAIL * (GI - 1 - slot)), tail.dtype)]
        return jnp.concatenate(parts, axis=1)

    for tap in range(4):
        taps = down_w[tap // 2, tap % 2].astype(F32)
        zeros = jnp.zeros((LANES - ch_in, 2 * LANES), BF16)
        for slot in range(GI):
            wd[slot, pl.ds(tap * LANES, ch_in), :LANES] = taps[:, :LANES].astype(BF16)
            wd[slot, pl.ds(tap * LANES, ch_in), LANES:] = tail_at(taps[:, LANES:], slot).astype(BF16)
            wd[slot, pl.ds(tap * LANES + ch_in, LANES - ch_in)] = zeros
    for k in range(2):
        for slot in range(GI):
            w1[k, slot, :LANES] = (pw1_w[k, :LANES, :].astype(F32) * HALF).astype(BF16)
            w1[k, slot, LANES:] = jnp.zeros((LANES, w1.shape[3]), BF16)
            w1[k, slot, pl.ds(LANES + TAIL * slot, TAIL)] = (pw1_w[k, LANES:, :].astype(F32) * HALF).astype(BF16)
            w2[k, slot, :LANES] = pw2_w[k, :LANES, :]
            w2[k, slot, LANES:] = jnp.zeros((LANES, w2.shape[3]), BF16)
            w2[k, slot, pl.ds(LANES + TAIL * slot, TAIL)] = pw2_w[k, LANES:, :]

    for kh in range(7):
        for kw in range(7):
            taps = dw_w[kh, kw].astype(F32)
            tails = jnp.concatenate([taps[:, LANES:]] * GI, axis=1)
            for k in range(2):
                dwf[k, 0, kh, kw:kw + 1] = taps[k:k + 1, :LANES]
                dwf[k, 1, kh, kw:kw + 1] = tails[k:k + 1]

    def split(row):
        row = row.astype(F32)
        return row[:, :LANES], jnp.concatenate([row[:, LANES:]] * GI, axis=1)

    names = [dw_b, norm_w, norm_b, pw2_b, layer_scale]
    for k in range(2):
        for j, ref in enumerate(names):
            head, tail = split(ref[k:k + 1, :])
            vec[k, 0, j:j + 1] = head
            vec[k, 1, j:j + 1] = tail
    head, tail = split(down_b[...].reshape(1, -1))
    vec[0, 0, 5:6] = head
    vec[0, 1, 5:6] = tail

    flat = pad.reshape(pad.shape[0], pad.shape[1] * ROW, LANES)

    def column(plane, row, col, count):
        return flat.at[plane, pl.ds((BORDER + row) * ROW + COL0 + col, count, stride=ROW), :]

    def messages(k, g):
        base = k * groups * NPL + g * NPL
        planes = pl.ds(base, NPL)
        copies = []
        for q, (dr, dc) in enumerate(steps):
            there = opposite(q)
            if dc == 0:
                first = BORDER if dr < 0 else tile_h
                land = BORDER + tile_h if dr < 0 else 0
                src = pad.at[planes, pl.ds(first, BORDER), pl.ds(COL0, tile_w), :]
                dst = pad.at[planes, pl.ds(land, BORDER), pl.ds(COL0, tile_w), :]
            elif dr == 0:
                src = hsend.at[k, g, q - 2]
                dst = hrecv.at[k, g, there - 2]
            else:
                src = csend.at[k, g, q - 4]
                dst = crecv.at[k, g, there - 4]
            copies.append(pltpu.make_async_remote_copy(
                src_ref=src, dst_ref=dst, send_sem=send_sem.at[k, g, q], recv_sem=recv_sem.at[k, g, there],
                device_id=device(q), device_id_type=MESH))
        return copies

    def send(k, g):
        base = k * groups * NPL + g * NPL
        copies = messages(k, g)
        for q in (2, 3):
            first = 0 if q == 2 else tile_w - BORDER

            def fill(p, _):
                for j in range(BORDER):
                    hsend[k, g, q - 2, p * BORDER + j] = column(base + p, 0, first + j, tile_h)[...].astype(BF16)
                return 0

            lax.fori_loop(0, NPL, fill, 0)
        for q in range(4, 8):
            dr, dc = steps[q]
            first = 0 if dc < 0 else tile_w - BORDER
            row = 0 if dr < 0 else tile_h - BORDER
            for p in range(NPL):
                for j in range(BORDER):
                    cstage[pl.ds((p * BORDER + j) * BORDER, BORDER)] = column(base + p, row, first + j, BORDER)[...]
            csend[k, g, q - 4] = cstage[...].astype(BF16)
        for q in range(8):
            pl.when(exists(q))(copies[q].start)

    def receive(k, g):
        base = k * groups * NPL + g * NPL
        for q in range(8):
            pl.when(exists(q))(_wait_recv(k, g, q))
        for q in (2, 3):
            first = -BORDER if q == 2 else tile_w

            @pl.when(exists(q))
            def _():
                def put(p, _):
                    for j in range(BORDER):
                        column(base + p, 0, first + j, tile_h)[...] = hrecv[k, g, q - 2, p * BORDER + j].astype(F32)
                    return 0

                lax.fori_loop(0, NPL, put, 0)
        for q in range(4, 8):
            dr, dc = steps[q]
            first = -BORDER if dc < 0 else tile_w
            row = -BORDER if dr < 0 else tile_h

            @pl.when(exists(q))
            def _():
                cstage[...] = crecv[k, g, q - 4].astype(F32)
                for p in range(NPL):
                    for j in range(BORDER):
                        column(base + p, row, first + j, BORDER)[...] = cstage[pl.ds((p * BORDER + j) * BORDER, BORDER)]

    def _wait_recv(k, g, q):
        base = k * groups * NPL + g * NPL
        dr, dc = steps[q]
        if dc == 0:
            land = 0 if dr < 0 else BORDER + tile_h
            dst = pad.at[pl.ds(base, NPL), pl.ds(land, BORDER), pl.ds(COL0, tile_w), :]
        elif dr == 0:
            dst = hrecv.at[k, g, q - 2]
        else:
            dst = crecv.at[k, g, q - 4]

        def wait():
            pltpu.make_async_remote_copy(
                src_ref=dst, dst_ref=dst, send_sem=send_sem.at[k, g, q], recv_sem=recv_sem.at[k, g, q],
                device_id=device(q), device_id_type=MESH).wait_recv()

        return wait

    def wait_send(k, g):
        copies = messages(k, g)
        for q in range(8):
            pl.when(exists(q))(copies[q].wait_send)

    def interior(plane):
        return pad.at[plane, pl.ds(BORDER, tile_h), pl.ds(COL0, tile_w), :]

    def rounded(values):
        return values.astype(BF16).astype(F32)

    def down_image(g, i):
        img = g * GI + i
        pltpu.make_async_copy(feat.at[img], fv.at[img], feat_sem.at[img]).wait()
        for w in range(in_w):
            x = fv[img, w].astype(F32)
            mean = jnp.sum(x, axis=0, keepdims=True) * (1.0 / ch_in)
            centered = x - mean
            var = jnp.sum(centered * centered, axis=0, keepdims=True) * (1.0 / ch_in)
            a = centered * lax.rsqrt(var + LN_EPS) * norm0[0, :, :in_h] + norm0[1, :, :in_h]
            ab[pl.ds(w * LANES, ch_in), :in_h] = a.astype(BF16)
        turned = lax.dot_general(sel[...], ab[...], (((1,), (1,)), ((), ())), preferred_element_type=F32).astype(BF16)
        taps = [jnp.concatenate([turned[:tile_h, w * 2 * LANES:(w + 1) * 2 * LANES], turned[tile_h:, w * 2 * LANES:(w + 1) * 2 * LANES]], axis=1) for w in range(tile_w)]
        d = jnp.dot(jnp.concatenate(taps, axis=0), wd[i], preferred_element_type=F32)
        head = rounded(d[:, :LANES] + vec[0, 0, 5:6])
        for w in range(tile_w):
            column(g * NPL + i, 0, w, tile_h)[...] = head[w * tile_h:(w + 1) * tile_h]
        return d[:, LANES:]

    def down_group(g, _):
        ybuf[...] = jnp.zeros(ybuf.shape, F32)

        def one(i, _):
            ybuf[...] += down_image(g, i)
            return 0

        lax.fori_loop(0, GI, one, 0)
        tail = rounded(ybuf[...] + vec[0, 1, 5:6])
        for w in range(tile_w):
            column(g * NPL + GI, 0, w, tile_h)[...] = tail[w * tile_h:(w + 1) * tile_h]

        @pl.when(g == 0)
        def _():
            count = jnp.int32(0)
            for q in range(8):
                count = count + exists(q).astype(jnp.int32)
            pl.semaphore_wait(barrier, count)

        send(0, g)
        return 0

    R = 16
    strips = tile_h // R

    def depthwise(k, g):
        base = k * groups * NPL + g * NPL

        def body(t, _):
            p, strip = t // strips, t % strips
            part = (p == GI).astype(jnp.int32)
            r0 = strip * R
            accs = [None] * R
            bias = vec[k, part, 0:1]
            for kw in range(7):
                xs = [pad[base + p, r0 + i, COL0 - BORDER + kw:COL0 - BORDER + kw + 8, :] for i in range(R + 6)]
                for kh in range(7):
                    w = jnp.broadcast_to(dwf[k, part, kh, kw:kw + 1, :], (8, LANES))
                    for r in range(R):
                        term = xs[r + kh] * w
                        accs[r] = term if accs[r] is None else accs[r] + term
            for r in range(R):
                ubuf[p, pl.ds((r0 + r) * 8, 8)] = accs[r] + bias
            return 0

        lax.fori_loop(0, NPL * strips, body, 0)

    LR = 64

    def norm(k):
        nw, nb = vec[k, 0, 1:2], vec[k, 0, 2:3]
        nwt, nbt = vec[k, 1, 1:2], vec[k, 1, 2:3]
        lane = lax.broadcasted_iota(jnp.int32, (LR, LANES), 1)
        channels = LANES + TAIL

        def body(t, _):
            rows = pl.ds(pl.multiple_of(t * LR, LR), LR)
            tail = ubuf[GI, rows]
            heads = [ubuf[i, rows] for i in range(GI)]
            own = [jnp.logical_and(lane >= i * TAIL, lane < (i + 1) * TAIL) for i in range(GI)]

            def pick(cols):
                res = cols[GI - 1]
                for i in range(GI - 2, -1, -1):
                    res = jnp.where(lane < (i + 1) * TAIL, cols[i], res)
                return res

            means = [jnp.sum(heads[i] + jnp.where(own[i], tail, 0.0), axis=-1, keepdims=True) * (1.0 / channels) for i in range(GI)]
            heads = [heads[i] - means[i] for i in range(GI)]
            tail = tail - pick(means)
            square = tail * tail
            rs = [lax.rsqrt(jnp.sum(heads[i] * heads[i] + jnp.where(own[i], square, 0.0), axis=-1, keepdims=True) * (1.0 / channels) + LN_EPS) for i in range(GI)]
            for i in range(GI):
                vbuf[i, rows] = (heads[i] * rs[i] * nw + nb).astype(BF16)
            vbuf[GI, rows] = (tail * pick(rs) * nwt + nbt).astype(BF16)
            return 0

        lax.fori_loop(0, pix // LR, body, 0)

    def mlp(k, g):
        base = k * groups * NPL + g * NPL
        nxt = groups * NPL + g * NPL
        b1 = pw1_b[k:k + 1, :].astype(F32) * HALF
        ybuf[...] = jnp.zeros(ybuf.shape, F32)

        def body(i, _):
            v = jnp.concatenate([vbuf[i], vbuf[GI]], axis=1)
            x = jnp.dot(v, w1[k, i], preferred_element_type=F32) + b1
            hidden = (x + x * lax.erf(x * RSQRT2X2)).astype(BF16)
            y = lax.dot_general(hidden, w2[k, i], (((1,), (1,)), ((), ())), preferred_element_type=F32)
            head = (y[:, :LANES] + vec[k, 0, 3:4]) * vec[k, 0, 4:5]
            ybuf[...] += y[:, LANES:]
            new = interior(base + i)[...] + head.reshape(tile_h, tile_w, LANES)
            if k == 0:
                interior(nxt + i)[...] = rounded(new)
            else:
                obuf[g * GI + i, :, :, :LANES] = new.astype(BF16)
            return 0

        lax.fori_loop(0, GI, body, 0)
        tail = ((ybuf[...] + vec[k, 1, 3:4]) * vec[k, 1, 4:5]).reshape(tile_h, tile_w, LANES)
        new = interior(base + GI)[...] + tail
        if k == 0:
            interior(nxt + GI)[...] = rounded(new)
        else:
            for i in range(GI):
                obuf[g * GI + i, :, :, LANES:] = new[:, :, i * TAIL:(i + 1) * TAIL].astype(BF16)

    def out_copy(g):
        imgs = pl.ds(g * GI, GI)
        return pltpu.make_async_copy(obuf.at[imgs], out.at[imgs], out_sem.at[g])

    def block_group(k):
        def body(g, _):
            receive(k, g)
            depthwise(k, g)
            norm(k)
            mlp(k, g)
            if k == 0:
                send(1, g)
            else:
                out_copy(g).start()
            return 0
        return body

    lax.fori_loop(0, groups, down_group, 0)
    lax.fori_loop(0, groups, block_group(0), 0)
    lax.fori_loop(0, groups, block_group(1), 0)

    def finish(g, _):
        wait_send(0, g)
        wait_send(1, g)
        out_copy(g).wait()
        return 0

    lax.fori_loop(0, groups, finish, 0)


def solution(mesh):
    rows_count = mesh.shape["sh"]
    cols_count = mesh.shape["sw"]
    act_spec = P("dp", "sh", "sw", None)

    def local_run(feat_map, norm0_w, norm0_b, down_w, down_b, dw_w, dw_b, norm_w, norm_b, pw1_w, pw1_b, pw2_w, pw2_b, layer_scale):
        images, in_h, in_w, ch_in = feat_map.shape
        tile_h, tile_w = in_h // 2, in_w // 2
        ch, hidden = pw1_w.shape[1:]
        groups = images // GI
        pix = tile_h * tile_w
        vmem = pl.BlockSpec(memory_space=pltpu.VMEM)
        hbm = pl.BlockSpec(memory_space=pl.ANY)
        return pl.pallas_call(
            functools.partial(kernel, rows_count, cols_count),
            out_shape=jax.ShapeDtypeStruct((images, tile_h, tile_w, ch), BF16),
            in_specs=[hbm] + [vmem] * 13,
            out_specs=hbm,
            scratch_shapes=[
                pltpu.VMEM((images, in_w, ch_in, in_h), BF16),
                pltpu.VMEM((in_w * LANES, LANES), BF16),
                pltpu.VMEM((in_h, LANES), BF16),
                pltpu.VMEM((2, ch_in, LANES), F32),
                pltpu.VMEM((2 * groups * NPL, tile_h + 2 * BORDER, ROW, LANES), F32),
                pltpu.VMEM((2, groups, 2, NPL * BORDER, tile_h, LANES), BF16),
                pltpu.VMEM((2, groups, 2, NPL * BORDER, tile_h, LANES), BF16),
                pltpu.VMEM((2, groups, 4, 48, LANES), BF16),
                pltpu.VMEM((2, groups, 4, 48, LANES), BF16),
                pltpu.VMEM((48, LANES), F32),
                pltpu.VMEM((NPL, pix, LANES), F32),
                pltpu.VMEM((NPL, pix, LANES), BF16),
                pltpu.VMEM((pix, LANES), F32),
                pltpu.VMEM((GI, 4 * LANES, 2 * LANES), BF16),
                pltpu.VMEM((2, GI, 2 * LANES, hidden), BF16),
                pltpu.VMEM((2, GI, 2 * LANES, hidden), BF16),
                pltpu.VMEM((2, 2, 7, 8, LANES), F32),
                pltpu.VMEM((2, 2, 8, LANES), F32),
                pltpu.VMEM((images, tile_h, tile_w, ch), BF16),
                pltpu.SemaphoreType.DMA((images,)),
                pltpu.SemaphoreType.DMA((groups,)),
                pltpu.SemaphoreType.DMA((2, groups, 8)),
                pltpu.SemaphoreType.DMA((2, groups, 8)),
            ],
            compiler_params=pltpu.CompilerParams(collective_id=0, has_side_effects=True, vmem_limit_bytes=63 * 1024 * 1024),
        )(
            feat_map.transpose(0, 2, 3, 1), norm0_w.reshape(1, -1), norm0_b.reshape(1, -1), down_w, down_b, dw_w.transpose(1, 2, 0, 3), dw_b,
            norm_w, norm_b, pw1_w, pw1_b, pw2_w.transpose(0, 2, 1), pw2_b, layer_scale,
        )

    return jax.shard_map(local_run, mesh=mesh, in_specs=(act_spec,) + (P(),) * 13, out_specs=act_spec, check_vma=False)
```

```python
import functools

import jax
import jax.numpy as jnp
from jax import lax
from jax.experimental import pallas as pl
from jax.experimental.pallas import tpu as pltpu
from jax.sharding import PartitionSpec as P

LN_EPS = 1e-6
MESH = pl.DeviceIdType.MESH
GI = 4
NPL = GI + 1
LANES = 128
TAIL = 32
ROW = 24
COL0 = 8
BORDER = 3
HALF = 0.5
RSQRT2X2 = 1.4142135623730951

F32 = jnp.float32
BF16 = jnp.bfloat16


def kernel(
    rows_count, cols_count,
    feat, norm0_w, norm0_b, down_w, down_b, dw_w, dw_b, norm_w, norm_b, pw1_w, pw1_b, pw2_w, pw2_b, layer_scale,
    out,
    fv, ab, sel, norm0, pad, hsend, hrecv, csend, crecv, cstage, ubuf, vbuf, ybuf, wd, wdt, pw1, pw2, w1, w1t, w2t, dwf, eye, diag, vec, obuf,
    feat_sem, weight_sem, out_sem, send_sem, recv_sem,
):
    images, in_w, ch_in, in_h = fv.shape
    groups = images // GI
    tile_h, tile_w = obuf.shape[1], obuf.shape[2]
    pix = tile_h * tile_w
    my_row, my_col = lax.axis_index("sh"), lax.axis_index("sw")
    has_up, has_down = my_row > 0, my_row < rows_count - 1
    has_left, has_right = my_col > 0, my_col < cols_count - 1

    steps = [(-1, 0), (1, 0), (0, -1), (0, 1), (-1, -1), (-1, 1), (1, -1), (1, 1)]
    row_ok = {-1: has_up, 0: None, 1: has_down}
    col_ok = {-1: has_left, 0: None, 1: has_right}

    def exists(q):
        dr, dc = steps[q]
        if row_ok[dr] is None:
            return col_ok[dc]
        if col_ok[dc] is None:
            return row_ok[dr]
        return jnp.logical_and(row_ok[dr], col_ok[dc])

    def opposite(q):
        dr, dc = steps[q]
        return steps.index((-dr, -dc))

    def device(q):
        dr, dc = steps[q]
        return {"sh": my_row + dr, "sw": my_col + dc}

    feat_copies = [pltpu.make_async_copy(feat.at[i], fv.at[i], feat_sem.at[i]) for i in range(images)]
    weight_copies = [pltpu.make_async_copy(pw1_w, pw1, weight_sem.at[0]), pltpu.make_async_copy(pw2_w, pw2, weight_sem.at[1])]
    for copy in feat_copies[:GI] + weight_copies + feat_copies[GI:]:
        copy.start()

    barrier = pltpu.get_barrier_semaphore()
    for q in range(8):
        @pl.when(exists(q))
        def _():
            pl.semaphore_signal(barrier, inc=1, device_id=device(q), device_id_type=MESH)

    def zero_rows(first):
        def body(p, _):
            pad[p, pl.ds(first, BORDER)] = jnp.zeros((BORDER, ROW, LANES), F32)
            return 0
        lax.fori_loop(0, pad.shape[0], body, 0)

    def zero_cols(first):
        def body(p, _):
            pad[p, :, pl.ds(first, 8)] = jnp.zeros((pad.shape[1], 8, LANES), F32)
            return 0
        lax.fori_loop(0, pad.shape[0], body, 0)

    pl.when(jnp.logical_not(has_up))(lambda: zero_rows(0))
    pl.when(jnp.logical_not(has_down))(lambda: zero_rows(BORDER + tile_h))
    pl.when(jnp.logical_not(has_left))(lambda: zero_cols(0))
    pl.when(jnp.logical_not(has_right))(lambda: zero_cols(COL0 + tile_w))

    ab[...] = jnp.zeros(ab.shape, BF16)
    row_id = lax.broadcasted_iota(jnp.int32, sel.shape, 0)
    col_id = lax.broadcasted_iota(jnp.int32, sel.shape, 1)
    picked = jnp.where(row_id < tile_h, 2 * row_id, 2 * (row_id - tile_h) + 1)
    sel[...] = jnp.where(col_id == picked, 1.0, 0.0).astype(BF16)
    norm0[0] = jnp.broadcast_to(norm0_w[...].astype(F32), (LANES, ch_in)).T
    norm0[1] = jnp.broadcast_to(norm0_b[...].astype(F32), (LANES, ch_in)).T
    cstage[...] = jnp.zeros(cstage.shape, F32)

    def tail_at(tail, slot):
        rows = tail.shape[0]
        parts = [tail]
        if slot:
            parts = [jnp.zeros((rows, TAIL * slot), tail.dtype)] + parts
        if slot < GI - 1:
            parts = parts + [jnp.zeros((rows, TAIL * (GI - 1 - slot)), tail.dtype)]
        return jnp.concatenate(parts, axis=1)

    for tap in range(4):
        taps = down_w[tap // 2, tap % 2].astype(F32)
        zeros = jnp.zeros((LANES - ch_in, LANES), BF16)
        wd[pl.ds(tap * LANES, ch_in)] = taps[:, :LANES].astype(BF16)
        wd[pl.ds(tap * LANES + ch_in, LANES - ch_in)] = zeros
        for slot in range(GI):
            wdt[slot, pl.ds(tap * LANES, ch_in)] = tail_at(taps[:, LANES:], slot).astype(BF16)
            wdt[slot, pl.ds(tap * LANES + ch_in, LANES - ch_in)] = zeros

    def block_weights():
        for copy in weight_copies:
            copy.wait()
        for k in range(2):
            w1[k] = (pw1[k, :LANES].astype(F32) * HALF).astype(BF16)
            up_tail = (pw1[k, LANES:].astype(F32) * HALF).astype(BF16)
            for slot in range(GI):
                for other in range(GI):
                    rows = pl.ds(TAIL * other, TAIL)
                    w1t[k, slot, rows] = up_tail if other == slot else jnp.zeros(up_tail.shape, BF16)
                    w2t[k, slot, rows] = pw2[k, LANES:] if other == slot else jnp.zeros(up_tail.shape, BF16)
        lax.fori_loop(0, 7, spread, 0)

    for kh in range(7):
        for kw in range(7):
            taps = dw_w[kh, kw].astype(F32)
            tails = jnp.concatenate([taps[:, LANES:]] * GI, axis=1)
            for k in range(2):
                dwf[k, 0, kh, kw:kw + 1] = taps[k:k + 1, :LANES]
                dwf[k, 1, kh, kw:kw + 1] = tails[k:k + 1]

    eye[...] = jnp.where(lax.broadcasted_iota(jnp.int32, eye.shape, 0) == lax.broadcasted_iota(jnp.int32, eye.shape, 1), 1.0, 0.0).astype(BF16)

    def spread(kw, _):
        unit = eye[...]
        for k in range(2):
            for kh in range(8):
                if kh < 7:
                    tap = jnp.broadcast_to(dwf[k, 0, kh, pl.ds(kw, 1)], (16, LANES)).astype(BF16)
                    block = unit * jnp.concatenate([tap] * (LANES // 16), axis=0)
                else:
                    block = jnp.zeros((LANES, LANES), BF16)
                diag[k, pl.ds(pl.multiple_of(kw * 4 * LANES, LANES) + kh // 2 * LANES, LANES), kh % 2 * LANES:(kh % 2 + 1) * LANES] = block
        return 0

    pad[:, tile_h + 2 * BORDER:] = jnp.zeros((pad.shape[0], 2, ROW, LANES), F32)

    def split(row):
        row = row.astype(F32)
        return row[:, :LANES], jnp.concatenate([row[:, LANES:]] * GI, axis=1)

    names = [dw_b, norm_w, norm_b, pw2_b, layer_scale]
    for k in range(2):
        for j, ref in enumerate(names):
            head, tail = split(ref[k:k + 1, :])
            vec[k, 0, j:j + 1] = head
            vec[k, 1, j:j + 1] = tail
    head, tail = split(down_b[...].reshape(1, -1))
    vec[0, 0, 5:6] = head
    vec[0, 1, 5:6] = tail

    flat = pad.reshape(pad.shape[0], pad.shape[1] * ROW, LANES)

    def column(plane, row, col, count):
        return flat.at[plane, pl.ds((BORDER + row) * ROW + COL0 + col, count, stride=ROW), :]

    def messages(k, g):
        base = k * groups * NPL + g * NPL
        planes = pl.ds(base, NPL)
        copies = []
        for q, (dr, dc) in enumerate(steps):
            there = opposite(q)
            if dc == 0:
                first = BORDER if dr < 0 else tile_h
                land = BORDER + tile_h if dr < 0 else 0
                src = pad.at[planes, pl.ds(first, BORDER), pl.ds(COL0, tile_w), :]
                dst = pad.at[planes, pl.ds(land, BORDER), pl.ds(COL0, tile_w), :]
            elif dr == 0:
                src = hsend.at[k, g, q - 2]
                dst = hrecv.at[k, g, there - 2]
            else:
                src = csend.at[k, g, q - 4]
                dst = crecv.at[k, g, there - 4]
            copies.append(pltpu.make_async_remote_copy(
                src_ref=src, dst_ref=dst, send_sem=send_sem.at[k, g, q], recv_sem=recv_sem.at[k, g, there],
                device_id=device(q), device_id_type=MESH))
        return copies

    def send(k, g):
        base = k * groups * NPL + g * NPL
        copies = messages(k, g)
        for q in (2, 3):
            first = 0 if q == 2 else tile_w - BORDER

            def fill(p, _):
                for j in range(BORDER):
                    hsend[k, g, q - 2, p * BORDER + j] = column(base + p, 0, first + j, tile_h)[...].astype(BF16)
                return 0

            lax.fori_loop(0, NPL, fill, 0)
        for q in range(4, 8):
            dr, dc = steps[q]
            first = 0 if dc < 0 else tile_w - BORDER
            row = 0 if dr < 0 else tile_h - BORDER
            for p in range(NPL):
                for j in range(BORDER):
                    cstage[pl.ds((p * BORDER + j) * BORDER, BORDER)] = column(base + p, row, first + j, BORDER)[...]
            csend[k, g, q - 4] = cstage[...].astype(BF16)
        for q in range(8):
            pl.when(exists(q))(copies[q].start)

    def receive(k, g):
        base = k * groups * NPL + g * NPL
        for q in range(8):
            pl.when(exists(q))(_wait_recv(k, g, q))
        for q in (2, 3):
            first = -BORDER if q == 2 else tile_w

            @pl.when(exists(q))
            def _():
                def put(p, _):
                    for j in range(BORDER):
                        column(base + p, 0, first + j, tile_h)[...] = hrecv[k, g, q - 2, p * BORDER + j].astype(F32)
                    return 0

                lax.fori_loop(0, NPL, put, 0)
        for q in range(4, 8):
            dr, dc = steps[q]
            first = -BORDER if dc < 0 else tile_w
            row = -BORDER if dr < 0 else tile_h

            @pl.when(exists(q))
            def _():
                cstage[...] = crecv[k, g, q - 4].astype(F32)
                for p in range(NPL):
                    for j in range(BORDER):
                        column(base + p, row, first + j, BORDER)[...] = cstage[pl.ds((p * BORDER + j) * BORDER, BORDER)]

    def _wait_recv(k, g, q):
        base = k * groups * NPL + g * NPL
        dr, dc = steps[q]
        if dc == 0:
            land = 0 if dr < 0 else BORDER + tile_h
            dst = pad.at[pl.ds(base, NPL), pl.ds(land, BORDER), pl.ds(COL0, tile_w), :]
        elif dr == 0:
            dst = hrecv.at[k, g, q - 2]
        else:
            dst = crecv.at[k, g, q - 4]

        def wait():
            pltpu.make_async_remote_copy(
                src_ref=dst, dst_ref=dst, send_sem=send_sem.at[k, g, q], recv_sem=recv_sem.at[k, g, q],
                device_id=device(q), device_id_type=MESH).wait_recv()

        return wait

    def wait_send(k, g):
        copies = messages(k, g)
        for q in range(8):
            pl.when(exists(q))(copies[q].wait_send)

    def interior(plane):
        return pad.at[plane, pl.ds(BORDER, tile_h), pl.ds(COL0, tile_w), :]

    def rounded(values):
        return values.astype(BF16).astype(F32)

    def down_norm(g, i, slot):
        img = g * GI + i
        pltpu.make_async_copy(feat.at[img], fv.at[img], feat_sem.at[img]).wait()
        for w in range(in_w):
            x = fv[img, w].astype(F32)
            mean = jnp.sum(x, axis=0, keepdims=True) * (1.0 / ch_in)
            centered = x - mean
            var = jnp.sum(centered * centered, axis=0, keepdims=True) * (1.0 / ch_in)
            a = centered * lax.rsqrt(var + LN_EPS) * norm0[0, :, :in_h] + norm0[1, :, :in_h]
            ab[slot, pl.ds(w * LANES, ch_in), :in_h] = a.astype(BF16)

    def down_conv(g, i, slot):
        turned = lax.dot_general(sel[...], ab[slot], (((1,), (1,)), ((), ())), preferred_element_type=F32).astype(BF16)
        taps = [jnp.concatenate([turned[:tile_h, w * 2 * LANES:(w + 1) * 2 * LANES], turned[tile_h:, w * 2 * LANES:(w + 1) * 2 * LANES]], axis=1) for w in range(tile_w)]
        weights = jnp.concatenate([wd[...], wdt[i]], axis=1)
        d = jnp.dot(jnp.concatenate(taps, axis=0), weights, preferred_element_type=F32)
        head = rounded(d[:, :LANES] + vec[0, 0, 5:6])
        for w in range(tile_w):
            column(g * NPL + i, 0, w, tile_h)[...] = head[w * tile_h:(w + 1) * tile_h]
        ybuf[...] += d[:, LANES:]

    def down_group(g, _):
        ybuf[...] = jnp.zeros(ybuf.shape, F32)

        def two(j, _):
            down_norm(g, 2 * j, 0)
            down_norm(g, 2 * j + 1, 1)
            down_conv(g, 2 * j, 0)
            down_conv(g, 2 * j + 1, 1)
            return 0

        lax.fori_loop(0, GI // 2, two, 0)
        tail = rounded(ybuf[...] + vec[0, 1, 5:6])
        for w in range(tile_w):
            column(g * NPL + GI, 0, w, tile_h)[...] = tail[w * tile_h:(w + 1) * tile_h]

        @pl.when(g == 0)
        def _():
            count = jnp.int32(0)
            for q in range(8):
                count = count + exists(q).astype(jnp.int32)
            pl.semaphore_wait(barrier, count)

        send(0, g)
        return 0

    half = tile_h // 2

    def taps_sum(k, part, plane, r0, count):
        accs = [None] * count
        for kw in range(7):
            xs = [pad[plane, r0 + i, COL0 - BORDER + kw:COL0 - BORDER + kw + 8, :] for i in range(count + 6)]
            for kh in range(7):
                w = jnp.broadcast_to(dwf[k, part, kh, kw:kw + 1, :], (8, LANES))
                for r in range(count):
                    term = xs[r + kh] * w
                    accs[r] = term if accs[r] is None else accs[r] + term
        return accs

    def depthwise(k, g):
        base = k * groups * NPL + g * NPL
        rows2 = (tile_h + 2) * tile_w

        def body(j, _):
            for strip in range(half // 12):
                r0 = j * half + strip * 12
                for r, acc in enumerate(taps_sum(k, 1, base + GI, r0, 12)):
                    ubuf[GI, pl.ds(pl.multiple_of((r0 + r) * 8, 8), 8)] = acc + vec[k, 1, 0:1]
            for strip in range(tile_h // 16):
                for r, acc in enumerate(taps_sum(k, 0, base + 2 + j, strip * 16, 16)):
                    ubuf[2 + j, pl.ds((strip * 16 + r) * 8, 8)] = acc + vec[k, 0, 0:1]

            parts = []
            for kw in range(0,7):
                shifted = pad[base + j, :, COL0 - BORDER + kw:COL0 - BORDER + kw + 8, :].astype(BF16).reshape(-1, LANES)
                for pair in range(4):
                    parts.append(shifted[pair * 16:pair * 16 + rows2])
            sums = jnp.dot(jnp.concatenate(parts, axis=1), diag[k, 0:3584], preferred_element_type=F32)
            part = sums[:pix, :LANES] + sums[8:pix + 8, LANES:]
            ubuf[j] = part + vec[k, 0, 0:1]
            return 0

        lax.fori_loop(0, 2, body, 0)

    LR = 64

    def norm(k):
        nw, nb = vec[k, 0, 1:2], vec[k, 0, 2:3]
        nwt, nbt = vec[k, 1, 1:2], vec[k, 1, 2:3]
        lane = lax.broadcasted_iota(jnp.int32, (LR, LANES), 1)
        channels = LANES + TAIL

        def body(t, _):
            rows = pl.ds(pl.multiple_of(t * LR, LR), LR)
            tail = ubuf[GI, rows]
            heads = [ubuf[i, rows] for i in range(GI)]
            own = [jnp.logical_and(lane >= i * TAIL, lane < (i + 1) * TAIL) for i in range(GI)]

            def pick(cols):
                res = cols[GI - 1]
                for i in range(GI - 2, -1, -1):
                    res = jnp.where(lane < (i + 1) * TAIL, cols[i], res)
                return res

            means = [jnp.sum(heads[i] + jnp.where(own[i], tail, 0.0), axis=-1, keepdims=True) * (1.0 / channels) for i in range(GI)]
            heads = [heads[i] - means[i] for i in range(GI)]
            tail = tail - pick(means)
            square = tail * tail
            rs = [lax.rsqrt(jnp.sum(heads[i] * heads[i] + jnp.where(own[i], square, 0.0), axis=-1, keepdims=True) * (1.0 / channels) + LN_EPS) for i in range(GI)]
            for i in range(GI):
                vbuf[i, rows] = (heads[i] * rs[i] * nw + nb).astype(BF16)
            vbuf[GI, rows] = (tail * pick(rs) * nwt + nbt).astype(BF16)
            return 0

        lax.fori_loop(0, pix // LR, body, 0)

    def mlp(k, g):
        base = k * groups * NPL + g * NPL
        nxt = groups * NPL + g * NPL
        b1 = pw1_b[k:k + 1, :].astype(F32) * HALF
        ybuf[...] = jnp.zeros(ybuf.shape, F32)

        def body(i, _):
            v = jnp.concatenate([vbuf[i], vbuf[GI]], axis=1)
            x = jnp.dot(v, jnp.concatenate([w1[k], w1t[k, i]], axis=0), preferred_element_type=F32) + b1
            hidden = (x + x * lax.erf(x * RSQRT2X2)).astype(BF16)
            y = lax.dot_general(hidden, jnp.concatenate([pw2[k, :LANES], w2t[k, i]], axis=0), (((1,), (1,)), ((), ())), preferred_element_type=F32)
            head = (y[:, :LANES] + vec[k, 0, 3:4]) * vec[k, 0, 4:5]
            ybuf[...] += y[:, LANES:]
            new = interior(base + i)[...] + head.reshape(tile_h, tile_w, LANES)
            if k == 0:
                interior(nxt + i)[...] = rounded(new)
            else:
                obuf[g * GI + i, :, :, :LANES] = new.astype(BF16)
            return 0

        lax.fori_loop(0, GI, body, 0)
        tail = ((ybuf[...] + vec[k, 1, 3:4]) * vec[k, 1, 4:5]).reshape(tile_h, tile_w, LANES)
        new = interior(base + GI)[...] + tail
        if k == 0:
            interior(nxt + GI)[...] = rounded(new)
        else:
            for i in range(GI):
                obuf[g * GI + i, :, :, LANES:] = new[:, :, i * TAIL:(i + 1) * TAIL].astype(BF16)

    def out_copy(g):
        imgs = pl.ds(g * GI, GI)
        return pltpu.make_async_copy(obuf.at[imgs], out.at[imgs], out_sem.at[g])

    def block_group(k):
        def body(g, _):
            receive(k, g)
            depthwise(k, g)
            norm(k)
            mlp(k, g)
            if k == 0:
                send(1, g)
            else:
                out_copy(g).start()
            return 0
        return body

    lax.fori_loop(0, groups, down_group, 0)
    block_weights()
    lax.fori_loop(0, groups, block_group(0), 0)
    lax.fori_loop(0, groups, block_group(1), 0)

    def finish(g, _):
        wait_send(0, g)
        wait_send(1, g)
        out_copy(g).wait()
        return 0

    lax.fori_loop(0, groups, finish, 0)


def solution(mesh):
    rows_count = mesh.shape["sh"]
    cols_count = mesh.shape["sw"]
    act_spec = P("dp", "sh", "sw", None)

    def local_run(feat_map, norm0_w, norm0_b, down_w, down_b, dw_w, dw_b, norm_w, norm_b, pw1_w, pw1_b, pw2_w, pw2_b, layer_scale):
        images, in_h, in_w, ch_in = feat_map.shape
        tile_h, tile_w = in_h // 2, in_w // 2
        ch, hidden = pw1_w.shape[1:]
        groups = images // GI
        pix = tile_h * tile_w
        vmem = pl.BlockSpec(memory_space=pltpu.VMEM)
        hbm = pl.BlockSpec(memory_space=pl.ANY)
        return pl.pallas_call(
            functools.partial(kernel, rows_count, cols_count),
            out_shape=jax.ShapeDtypeStruct((images, tile_h, tile_w, ch), BF16),
            in_specs=[hbm] + [vmem] * 8 + [hbm, vmem, hbm, vmem, vmem],
            out_specs=hbm,
            scratch_shapes=[
                pltpu.VMEM((images, in_w, ch_in, in_h), BF16),
                pltpu.VMEM((2, in_w * LANES, LANES), BF16),
                pltpu.VMEM((in_h, LANES), BF16),
                pltpu.VMEM((2, ch_in, LANES), F32),
                pltpu.VMEM((2 * groups * NPL, tile_h + 2 * BORDER + 2, ROW, LANES), F32),
                pltpu.VMEM((2, groups, 2, NPL * BORDER, tile_h, LANES), BF16),
                pltpu.VMEM((2, groups, 2, NPL * BORDER, tile_h, LANES), BF16),
                pltpu.VMEM((2, groups, 4, 48, LANES), BF16),
                pltpu.VMEM((2, groups, 4, 48, LANES), BF16),
                pltpu.VMEM((48, LANES), F32),
                pltpu.VMEM((NPL, pix, LANES), F32),
                pltpu.VMEM((NPL, pix, LANES), BF16),
                pltpu.VMEM((pix, LANES), F32),
                pltpu.VMEM((4 * LANES, LANES), BF16),
                pltpu.VMEM((GI, 4 * LANES, LANES), BF16),
                pltpu.VMEM((2, ch, hidden), BF16),
                pltpu.VMEM((2, ch, hidden), BF16),
                pltpu.VMEM((2, LANES, hidden), BF16),
                pltpu.VMEM((2, GI, LANES, hidden), BF16),
                pltpu.VMEM((2, GI, LANES, hidden), BF16),
                pltpu.VMEM((2, 2, 7, 8, LANES), F32),
                pltpu.VMEM((LANES, LANES), BF16),
                pltpu.VMEM((2, 7 * 4 * LANES, 2 * LANES), BF16),
                pltpu.VMEM((2, 2, 8, LANES), F32),
                pltpu.VMEM((images, tile_h, tile_w, ch), BF16),
                pltpu.SemaphoreType.DMA((images,)),
                pltpu.SemaphoreType.DMA((2,)),
                pltpu.SemaphoreType.DMA((groups,)),
                pltpu.SemaphoreType.DMA((2, groups, 8)),
                pltpu.SemaphoreType.DMA((2, groups, 8)),
            ],
            compiler_params=pltpu.CompilerParams(collective_id=0, has_side_effects=True, vmem_limit_bytes=63 * 1024 * 1024),
        )(
            feat_map.transpose(0, 2, 3, 1), norm0_w.reshape(1, -1), norm0_b.reshape(1, -1), down_w, down_b, dw_w.transpose(1, 2, 0, 3), dw_b,
            norm_w, norm_b, pw1_w, pw1_b, pw2_w.transpose(0, 2, 1), pw2_b, layer_scale,
        )

    return jax.shard_map(local_run, mesh=mesh, in_specs=(act_spec,) + (P(),) * 13, out_specs=act_spec, check_vma=False)
```

```python
import functools

import jax
import jax.numpy as jnp
from jax import lax
from jax.experimental import pallas as pl
from jax.experimental.pallas import tpu as pltpu
from jax.sharding import PartitionSpec as P

LN_EPS = 1e-6
MESH = pl.DeviceIdType.MESH
GI = 4
NPL = GI + 1
LANES = 128
TAIL = 32
ROW = 24
COL0 = 8
BORDER = 3
HALF = 0.5
RSQRT2X2 = 1.4142135623730951

F32 = jnp.float32
BF16 = jnp.bfloat16


def kernel(
    rows_count, cols_count,
    feat, norm0_w, norm0_b, down_w, down_b, dw_w, dw_b, norm_w, norm_b, pw1_w, pw1_b, pw2_w, pw2_b, layer_scale,
    out,
    fv, ab, sel, norm0, pad, hsend, hrecv, csend, crecv, cstage, ubuf, vbuf, ybuf, wd, wdt, pw1, pw2, w1, w1t, w2t, dwf, eye, diag, vec, obuf,
    feat_sem, weight_sem, out_sem, send_sem, recv_sem,
):
    images, in_w, ch_in, in_h = fv.shape
    groups = images // GI
    tile_h, tile_w = obuf.shape[1], obuf.shape[2]
    pix = tile_h * tile_w
    my_row, my_col = lax.axis_index("sh"), lax.axis_index("sw")
    has_up, has_down = my_row > 0, my_row < rows_count - 1
    has_left, has_right = my_col > 0, my_col < cols_count - 1

    steps = [(-1, 0), (1, 0), (0, -1), (0, 1), (-1, -1), (-1, 1), (1, -1), (1, 1)]
    row_ok = {-1: has_up, 0: None, 1: has_down}
    col_ok = {-1: has_left, 0: None, 1: has_right}

    def exists(q):
        dr, dc = steps[q]
        if row_ok[dr] is None:
            return col_ok[dc]
        if col_ok[dc] is None:
            return row_ok[dr]
        return jnp.logical_and(row_ok[dr], col_ok[dc])

    def opposite(q):
        dr, dc = steps[q]
        return steps.index((-dr, -dc))

    def device(q):
        dr, dc = steps[q]
        return {"sh": my_row + dr, "sw": my_col + dc}

    feat_copies = [pltpu.make_async_copy(feat.at[i], fv.at[i], feat_sem.at[i]) for i in range(images)]
    weight_copies = [pltpu.make_async_copy(pw1_w, pw1, weight_sem.at[0]), pltpu.make_async_copy(pw2_w, pw2, weight_sem.at[1])]
    for copy in feat_copies[:GI] + weight_copies + feat_copies[GI:]:
        copy.start()

    barrier = pltpu.get_barrier_semaphore()
    for q in range(8):
        @pl.when(exists(q))
        def _():
            pl.semaphore_signal(barrier, inc=1, device_id=device(q), device_id_type=MESH)

    def zero_rows(first):
        def body(p, _):
            pad[p, pl.ds(first, BORDER)] = jnp.zeros((BORDER, ROW, LANES), F32)
            return 0
        lax.fori_loop(0, pad.shape[0], body, 0)

    def zero_cols(first):
        def body(p, _):
            pad[p, :, pl.ds(first, 8)] = jnp.zeros((pad.shape[1], 8, LANES), F32)
            return 0
        lax.fori_loop(0, pad.shape[0], body, 0)

    pl.when(jnp.logical_not(has_up))(lambda: zero_rows(0))
    pl.when(jnp.logical_not(has_down))(lambda: zero_rows(BORDER + tile_h))
    pl.when(jnp.logical_not(has_left))(lambda: zero_cols(0))
    pl.when(jnp.logical_not(has_right))(lambda: zero_cols(COL0 + tile_w))

    ab[...] = jnp.zeros(ab.shape, BF16)
    row_id = lax.broadcasted_iota(jnp.int32, sel.shape, 0)
    col_id = lax.broadcasted_iota(jnp.int32, sel.shape, 1)
    picked = jnp.where(row_id < tile_h, 2 * row_id, 2 * (row_id - tile_h) + 1)
    sel[...] = jnp.where(col_id == picked, 1.0, 0.0).astype(BF16)
    norm0[0] = jnp.broadcast_to(norm0_w[...].astype(F32), (LANES, ch_in)).T
    norm0[1] = jnp.broadcast_to(norm0_b[...].astype(F32), (LANES, ch_in)).T
    cstage[...] = jnp.zeros(cstage.shape, F32)

    def tail_at(tail, slot):
        rows = tail.shape[0]
        parts = [tail]
        if slot:
            parts = [jnp.zeros((rows, TAIL * slot), tail.dtype)] + parts
        if slot < GI - 1:
            parts = parts + [jnp.zeros((rows, TAIL * (GI - 1 - slot)), tail.dtype)]
        return jnp.concatenate(parts, axis=1)

    for tap in range(4):
        taps = down_w[tap // 2, tap % 2].astype(F32)
        zeros = jnp.zeros((LANES - ch_in, LANES), BF16)
        wd[pl.ds(tap * LANES, ch_in)] = taps[:, :LANES].astype(BF16)
        wd[pl.ds(tap * LANES + ch_in, LANES - ch_in)] = zeros
        for slot in range(GI):
            wdt[slot, pl.ds(tap * LANES, ch_in)] = tail_at(taps[:, LANES:], slot).astype(BF16)
            wdt[slot, pl.ds(tap * LANES + ch_in, LANES - ch_in)] = zeros

    def block_weights():
        for copy in weight_copies:
            copy.wait()
        for k in range(2):
            w1[k] = (pw1[k, :LANES].astype(F32) * HALF).astype(BF16)
            up_tail = (pw1[k, LANES:].astype(F32) * HALF).astype(BF16)
            for slot in range(GI):
                for other in range(GI):
                    rows = pl.ds(TAIL * other, TAIL)
                    w1t[k, slot, rows] = up_tail if other == slot else jnp.zeros(up_tail.shape, BF16)
                    w2t[k, slot, rows] = pw2[k, LANES:] if other == slot else jnp.zeros(up_tail.shape, BF16)
        lax.fori_loop(0, 7, spread, 0)

    for kh in range(7):
        for kw in range(7):
            taps = dw_w[kh, kw].astype(F32)
            tails = jnp.concatenate([taps[:, LANES:]] * GI, axis=1)
            for k in range(2):
                dwf[k, 0, kh, kw:kw + 1] = taps[k:k + 1, :LANES]
                dwf[k, 1, kh, kw:kw + 1] = tails[k:k + 1]

    eye[...] = jnp.where(lax.broadcasted_iota(jnp.int32, eye.shape, 0) == lax.broadcasted_iota(jnp.int32, eye.shape, 1), 1.0, 0.0).astype(BF16)

    def spread(kw, _):
        unit = eye[...]
        for k in range(2):
            for kh in range(8):
                if kh < 7:
                    tap = jnp.broadcast_to(dwf[k, 0, kh, pl.ds(kw, 1)], (16, LANES)).astype(BF16)
                    block = unit * jnp.concatenate([tap] * (LANES // 16), axis=0)
                else:
                    block = jnp.zeros((LANES, LANES), BF16)
                diag[k, pl.ds(pl.multiple_of(kw * 4 * LANES, LANES) + kh // 2 * LANES, LANES), kh % 2 * LANES:(kh % 2 + 1) * LANES] = block
        return 0

    pad[:, tile_h + 2 * BORDER:] = jnp.zeros((pad.shape[0], 2, ROW, LANES), F32)

    def split(row):
        row = row.astype(F32)
        return row[:, :LANES], jnp.concatenate([row[:, LANES:]] * GI, axis=1)

    names = [dw_b, norm_w, norm_b, pw2_b, layer_scale]
    for k in range(2):
        for j, ref in enumerate(names):
            head, tail = split(ref[k:k + 1, :])
            vec[k, 0, j:j + 1] = head
            vec[k, 1, j:j + 1] = tail
    head, tail = split(down_b[...].reshape(1, -1))
    vec[0, 0, 5:6] = head
    vec[0, 1, 5:6] = tail

    flat = pad.reshape(pad.shape[0], pad.shape[1] * ROW, LANES)

    def column(plane, row, col, count):
        return flat.at[plane, pl.ds((BORDER + row) * ROW + COL0 + col, count, stride=ROW), :]

    def messages(k, g):
        base = k * groups * NPL + g * NPL
        planes = pl.ds(base, NPL)
        copies = []
        for q, (dr, dc) in enumerate(steps):
            there = opposite(q)
            if dc == 0:
                first = BORDER if dr < 0 else tile_h
                land = BORDER + tile_h if dr < 0 else 0
                src = pad.at[planes, pl.ds(first, BORDER), pl.ds(COL0, tile_w), :]
                dst = pad.at[planes, pl.ds(land, BORDER), pl.ds(COL0, tile_w), :]
            elif dr == 0:
                src = hsend.at[k, g, q - 2]
                dst = hrecv.at[k, g, there - 2]
            else:
                src = csend.at[k, g, q - 4]
                dst = crecv.at[k, g, there - 4]
            copies.append(pltpu.make_async_remote_copy(
                src_ref=src, dst_ref=dst, send_sem=send_sem.at[k, g, q], recv_sem=recv_sem.at[k, g, there],
                device_id=device(q), device_id_type=MESH))
        return copies

    def send(k, g):
        base = k * groups * NPL + g * NPL
        copies = messages(k, g)
        for q in (2, 3):
            first = 0 if q == 2 else tile_w - BORDER

            def fill(p, _):
                for j in range(BORDER):
                    hsend[k, g, q - 2, p * BORDER + j] = column(base + p, 0, first + j, tile_h)[...].astype(BF16)
                return 0

            lax.fori_loop(0, NPL, fill, 0)
        for q in range(4, 8):
            dr, dc = steps[q]
            first = 0 if dc < 0 else tile_w - BORDER
            row = 0 if dr < 0 else tile_h - BORDER
            for p in range(NPL):
                for j in range(BORDER):
                    cstage[pl.ds((p * BORDER + j) * BORDER, BORDER)] = column(base + p, row, first + j, BORDER)[...]
            csend[k, g, q - 4] = cstage[...].astype(BF16)
        for q in range(8):
            pl.when(exists(q))(copies[q].start)

    def receive(k, g):
        base = k * groups * NPL + g * NPL
        for q in range(8):
            pl.when(exists(q))(_wait_recv(k, g, q))
        for q in (2, 3):
            first = -BORDER if q == 2 else tile_w

            @pl.when(exists(q))
            def _():
                def put(p, _):
                    for j in range(BORDER):
                        column(base + p, 0, first + j, tile_h)[...] = hrecv[k, g, q - 2, p * BORDER + j].astype(F32)
                    return 0

                lax.fori_loop(0, NPL, put, 0)
        for q in range(4, 8):
            dr, dc = steps[q]
            first = -BORDER if dc < 0 else tile_w
            row = -BORDER if dr < 0 else tile_h

            @pl.when(exists(q))
            def _():
                cstage[...] = crecv[k, g, q - 4].astype(F32)
                for p in range(NPL):
                    for j in range(BORDER):
                        column(base + p, row, first + j, BORDER)[...] = cstage[pl.ds((p * BORDER + j) * BORDER, BORDER)]

    def _wait_recv(k, g, q):
        base = k * groups * NPL + g * NPL
        dr, dc = steps[q]
        if dc == 0:
            land = 0 if dr < 0 else BORDER + tile_h
            dst = pad.at[pl.ds(base, NPL), pl.ds(land, BORDER), pl.ds(COL0, tile_w), :]
        elif dr == 0:
            dst = hrecv.at[k, g, q - 2]
        else:
            dst = crecv.at[k, g, q - 4]

        def wait():
            pltpu.make_async_remote_copy(
                src_ref=dst, dst_ref=dst, send_sem=send_sem.at[k, g, q], recv_sem=recv_sem.at[k, g, q],
                device_id=device(q), device_id_type=MESH).wait_recv()

        return wait

    def wait_send(k, g):
        copies = messages(k, g)
        for q in range(8):
            pl.when(exists(q))(copies[q].wait_send)

    def interior(plane):
        return pad.at[plane, pl.ds(BORDER, tile_h), pl.ds(COL0, tile_w), :]

    def rounded(values):
        return values.astype(BF16).astype(F32)

    def down_norm(g, i, slot):
        img = g * GI + i
        pltpu.make_async_copy(feat.at[img], fv.at[img], feat_sem.at[img]).wait()
        for w in range(in_w):
            x = fv[img, w].astype(F32)
            mean = jnp.sum(x, axis=0, keepdims=True) * (1.0 / ch_in)
            centered = x - mean
            var = jnp.sum(centered * centered, axis=0, keepdims=True) * (1.0 / ch_in)
            a = centered * lax.rsqrt(var + LN_EPS) * norm0[0, :, :in_h] + norm0[1, :, :in_h]
            ab[slot, pl.ds(w * LANES, ch_in), :in_h] = a.astype(BF16)

    def down_conv(g, i, slot):
        turned = lax.dot_general(sel[...], ab[slot], (((1,), (1,)), ((), ())), preferred_element_type=F32).astype(BF16)
        taps = [jnp.concatenate([turned[:tile_h, w * 2 * LANES:(w + 1) * 2 * LANES], turned[tile_h:, w * 2 * LANES:(w + 1) * 2 * LANES]], axis=1) for w in range(tile_w)]
        weights = jnp.concatenate([wd[...], wdt[i]], axis=1)
        d = jnp.dot(jnp.concatenate(taps, axis=0), weights, preferred_element_type=F32)
        head = rounded(d[:, :LANES] + vec[0, 0, 5:6])
        for w in range(tile_w):
            column(g * NPL + i, 0, w, tile_h)[...] = head[w * tile_h:(w + 1) * tile_h]
        ybuf[...] += d[:, LANES:]

    def down_group(g, _):
        ybuf[...] = jnp.zeros(ybuf.shape, F32)

        def two(j, _):
            down_norm(g, 2 * j, 0)
            down_norm(g, 2 * j + 1, 1)
            down_conv(g, 2 * j, 0)
            down_conv(g, 2 * j + 1, 1)
            return 0

        lax.fori_loop(0, GI // 2, two, 0)
        tail = rounded(ybuf[...] + vec[0, 1, 5:6])
        for w in range(tile_w):
            column(g * NPL + GI, 0, w, tile_h)[...] = tail[w * tile_h:(w + 1) * tile_h]

        @pl.when(g == 0)
        def _():
            count = jnp.int32(0)
            for q in range(8):
                count = count + exists(q).astype(jnp.int32)
            pl.semaphore_wait(barrier, count)

        send(0, g)
        return 0

    half = tile_h // 2

    def taps_sum(k, part, plane, r0, count):
        accs = [None] * count
        for kw in range(7):
            xs = [pad[plane, r0 + i, COL0 - BORDER + kw:COL0 - BORDER + kw + 8, :] for i in range(count + 6)]
            for kh in range(7):
                w = jnp.broadcast_to(dwf[k, part, kh, kw:kw + 1, :], (8, LANES))
                for r in range(count):
                    term = xs[r + kh] * w
                    accs[r] = term if accs[r] is None else accs[r] + term
        return accs

    def depthwise(k, g):
        base = k * groups * NPL + g * NPL
        rows2 = (tile_h + 2) * tile_w

        def body(j, _):
            for strip in range(half // 12):
                r0 = j * half + strip * 12
                for r, acc in enumerate(taps_sum(k, 1, base + GI, r0, 12)):
                    ubuf[GI, pl.ds(pl.multiple_of((r0 + r) * 8, 8), 8)] = acc + vec[k, 1, 0:1]
            for strip in range(tile_h // 16):
                for r, acc in enumerate(taps_sum(k, 0, base + 2 + j, strip * 16, 16)):
                    ubuf[2 + j, pl.ds((strip * 16 + r) * 8, 8)] = acc + vec[k, 0, 0:1]

            parts = []
            for kw in range(0,7):
                shifted = pad[base + j, :, COL0 - BORDER + kw:COL0 - BORDER + kw + 8, :].astype(BF16).reshape(-1, LANES)
                for pair in range(4):
                    parts.append(shifted[pair * 16:pair * 16 + rows2])
            sums = jnp.dot(jnp.concatenate(parts, axis=1), diag[k, 0:3584], preferred_element_type=F32)
            part = sums[:pix, :LANES] + sums[8:pix + 8, LANES:]
            ubuf[j] = part + vec[k, 0, 0:1]
            return 0

        lax.fori_loop(0, 2, body, 0)

    LR = 64

    def norm(k):
        nw, nb = vec[k, 0, 1:2], vec[k, 0, 2:3]
        nwt, nbt = vec[k, 1, 1:2], vec[k, 1, 2:3]
        lane = lax.broadcasted_iota(jnp.int32, (LR, LANES), 1)
        channels = LANES + TAIL

        def body(t, _):
            rows = pl.ds(t * LR, LR)
            tail = ubuf[GI, rows]
            heads = [ubuf[i, rows] for i in range(GI)]
            own = [jnp.logical_and(lane >= i * TAIL, lane < (i + 1) * TAIL) for i in range(GI)]

            def pick(cols):
                res = cols[GI - 1]
                for i in range(GI - 2, -1, -1):
                    res = jnp.where(lane < (i + 1) * TAIL, cols[i], res)
                return res

            means = [jnp.sum(heads[i] + jnp.where(own[i], tail, 0.0), axis=-1, keepdims=True) * (1.0 / channels) for i in range(GI)]
            heads = [heads[i] - means[i] for i in range(GI)]
            tail = tail - pick(means)
            square = tail * tail
            rs = [lax.rsqrt(jnp.sum(heads[i] * heads[i] + jnp.where(own[i], square, 0.0), axis=-1, keepdims=True) * (1.0 / channels) + LN_EPS) for i in range(GI)]
            for i in range(GI):
                vbuf[i, rows] = (heads[i] * rs[i] * nw + nb).astype(BF16)
            vbuf[GI, rows] = (tail * pick(rs) * nwt + nbt).astype(BF16)
            return 0

        for t in range(pix // LR):
            body(t, 0)

    def mlp(k, g):
        base = k * groups * NPL + g * NPL
        nxt = groups * NPL + g * NPL
        b1 = pw1_b[k:k + 1, :].astype(F32) * HALF
        def up(i):
            v = jnp.concatenate([vbuf[i], vbuf[GI]], axis=1)
            return jnp.dot(v, jnp.concatenate([w1[k], w1t[k, i]], axis=0), preferred_element_type=F32)

        def act(x):
            x = x + b1
            return (x + x * lax.erf(x * RSQRT2X2)).astype(BF16)

        def down(i, hidden):
            y = lax.dot_general(hidden, jnp.concatenate([pw2[k, :LANES], w2t[k, i]], axis=0), (((1,), (1,)), ((), ())), preferred_element_type=F32)
            head = (y[:, :LANES] + vec[k, 0, 3:4]) * vec[k, 0, 4:5]
            new = interior(base + i)[...] + head.reshape(tile_h, tile_w, LANES)
            if k == 0:
                interior(nxt + i)[...] = rounded(new)
            else:
                obuf[g * GI + i, :, :, :LANES] = new.astype(BF16)
            return y[:, LANES:]

        x = up(0)
        for i in range(GI):
            hidden = act(x)
            if i < GI - 1:
                x = up(i + 1)
            tail = down(i, hidden)
            ybuf[...] = tail if i == 0 else ybuf[...] + tail
        tail = ((ybuf[...] + vec[k, 1, 3:4]) * vec[k, 1, 4:5]).reshape(tile_h, tile_w, LANES)
        new = interior(base + GI)[...] + tail
        if k == 0:
            interior(nxt + GI)[...] = rounded(new)
        else:
            for i in range(GI):
                obuf[g * GI + i, :, :, LANES:] = new[:, :, i * TAIL:(i + 1) * TAIL].astype(BF16)

    def out_copy(g):
        imgs = pl.ds(g * GI, GI)
        return pltpu.make_async_copy(obuf.at[imgs], out.at[imgs], out_sem.at[g])

    def block_group(k):
        def body(g, _):
            receive(k, g)
            depthwise(k, g)
            norm(k)
            mlp(k, g)
            if k == 0:
                send(1, g)
            else:
                out_copy(g).start()
            return 0
        return body

    lax.fori_loop(0, groups, down_group, 0)
    block_weights()
    lax.fori_loop(0, groups, block_group(0), 0)
    lax.fori_loop(0, groups, block_group(1), 0)

    def finish(g, _):
        wait_send(0, g)
        wait_send(1, g)
        out_copy(g).wait()
        return 0

    lax.fori_loop(0, groups, finish, 0)


def solution(mesh):
    rows_count = mesh.shape["sh"]
    cols_count = mesh.shape["sw"]
    act_spec = P("dp", "sh", "sw", None)

    def local_run(feat_map, norm0_w, norm0_b, down_w, down_b, dw_w, dw_b, norm_w, norm_b, pw1_w, pw1_b, pw2_w, pw2_b, layer_scale):
        images, in_h, in_w, ch_in = feat_map.shape
        tile_h, tile_w = in_h // 2, in_w // 2
        ch, hidden = pw1_w.shape[1:]
        groups = images // GI
        pix = tile_h * tile_w
        vmem = pl.BlockSpec(memory_space=pltpu.VMEM)
        hbm = pl.BlockSpec(memory_space=pl.ANY)
        return pl.pallas_call(
            functools.partial(kernel, rows_count, cols_count),
            out_shape=jax.ShapeDtypeStruct((images, tile_h, tile_w, ch), BF16),
            in_specs=[hbm] + [vmem] * 8 + [hbm, vmem, hbm, vmem, vmem],
            out_specs=hbm,
            scratch_shapes=[
                pltpu.VMEM((images, in_w, ch_in, in_h), BF16),
                pltpu.VMEM((2, in_w * LANES, LANES), BF16),
                pltpu.VMEM((in_h, LANES), BF16),
                pltpu.VMEM((2, ch_in, LANES), F32),
                pltpu.VMEM((2 * groups * NPL, tile_h + 2 * BORDER + 2, ROW, LANES), F32),
                pltpu.VMEM((2, groups, 2, NPL * BORDER, tile_h, LANES), BF16),
                pltpu.VMEM((2, groups, 2, NPL * BORDER, tile_h, LANES), BF16),
                pltpu.VMEM((2, groups, 4, 48, LANES), BF16),
                pltpu.VMEM((2, groups, 4, 48, LANES), BF16),
                pltpu.VMEM((48, LANES), F32),
                pltpu.VMEM((NPL, pix, LANES), F32),
                pltpu.VMEM((NPL, pix, LANES), BF16),
                pltpu.VMEM((pix, LANES), F32),
                pltpu.VMEM((4 * LANES, LANES), BF16),
                pltpu.VMEM((GI, 4 * LANES, LANES), BF16),
                pltpu.VMEM((2, ch, hidden), BF16),
                pltpu.VMEM((2, ch, hidden), BF16),
                pltpu.VMEM((2, LANES, hidden), BF16),
                pltpu.VMEM((2, GI, LANES, hidden), BF16),
                pltpu.VMEM((2, GI, LANES, hidden), BF16),
                pltpu.VMEM((2, 2, 7, 8, LANES), F32),
                pltpu.VMEM((LANES, LANES), BF16),
                pltpu.VMEM((2, 7 * 4 * LANES, 2 * LANES), BF16),
                pltpu.VMEM((2, 2, 8, LANES), F32),
                pltpu.VMEM((images, tile_h, tile_w, ch), BF16),
                pltpu.SemaphoreType.DMA((images,)),
                pltpu.SemaphoreType.DMA((2,)),
                pltpu.SemaphoreType.DMA((groups,)),
                pltpu.SemaphoreType.DMA((2, groups, 8)),
                pltpu.SemaphoreType.DMA((2, groups, 8)),
            ],
            compiler_params=pltpu.CompilerParams(collective_id=0, has_side_effects=True, vmem_limit_bytes=63 * 1024 * 1024),
        )(
            feat_map.transpose(0, 2, 3, 1), norm0_w.reshape(1, -1), norm0_b.reshape(1, -1), down_w, down_b, dw_w.transpose(1, 2, 0, 3), dw_b,
            norm_w, norm_b, pw1_w, pw1_b, pw2_w.transpose(0, 2, 1), pw2_b, layer_scale,
        )

    return jax.shard_map(local_run, mesh=mesh, in_specs=(act_spec,) + (P(),) * 13, out_specs=act_spec, check_vma=False)
```

```python
import functools

import jax
import jax.numpy as jnp
from jax import lax
from jax.experimental import pallas as pl
from jax.experimental.pallas import tpu as pltpu
from jax.sharding import PartitionSpec as P

LN_EPS = 1e-6
MESH = pl.DeviceIdType.MESH
GI = 4
NPL = GI + 1
LANES = 128
TAIL = 32
ROW = 24
COL0 = 8
BORDER = 3
HALF = 0.5
RSQRT2X2 = 1.4142135623730951

F32 = jnp.float32
BF16 = jnp.bfloat16


def kernel(
    rows_count, cols_count,
    feat, norm0_w_hbm, norm0_b_hbm, down_w_hbm, down_b_hbm, dw_w_hbm, dw_b_hbm, norm_w_hbm, norm_b_hbm, pw1_w_hbm, pw1_b_hbm, pw2_w_hbm, pw2_b_hbm, scale_hbm,
    out,
    norm0_w, norm0_b, down_w, down_b, dw_w, dw_b, norm_w, norm_b, pw1, pw1_b, pw2, pw2_b, layer_scale,
    fv, ab, sel, norm0, pad, hsend, hrecv, csend, crecv, cstage, ubuf, vbuf, ybuf, wd, wdt, w1, w1t, w2t, dwf, eye, diag, vec, obuf,
    feat_sem, weight_sem, out_sem, send_sem, recv_sem,
):
    images, in_w, ch_in, in_h = fv.shape
    groups = images // GI
    tile_h, tile_w = obuf.shape[1], obuf.shape[2]
    pix = tile_h * tile_w
    my_row, my_col = lax.axis_index("sh"), lax.axis_index("sw")
    has_up, has_down = my_row > 0, my_row < rows_count - 1
    has_left, has_right = my_col > 0, my_col < cols_count - 1

    steps = [(-1, 0), (1, 0), (0, -1), (0, 1), (-1, -1), (-1, 1), (1, -1), (1, 1)]
    row_ok = {-1: has_up, 0: None, 1: has_down}
    col_ok = {-1: has_left, 0: None, 1: has_right}

    def exists(q):
        dr, dc = steps[q]
        if row_ok[dr] is None:
            return col_ok[dc]
        if col_ok[dc] is None:
            return row_ok[dr]
        return jnp.logical_and(row_ok[dr], col_ok[dc])

    def opposite(q):
        dr, dc = steps[q]
        return steps.index((-dr, -dc))

    def device(q):
        dr, dc = steps[q]
        return {"sh": my_row + dr, "sw": my_col + dc}

    feat_copies = [pltpu.make_async_copy(feat.at[i], fv.at[i], feat_sem.at[i]) for i in range(images)]
    weights_hbm = [norm0_w_hbm, norm0_b_hbm, down_w_hbm, down_b_hbm, dw_w_hbm, dw_b_hbm, norm_w_hbm, norm_b_hbm, pw1_w_hbm, pw1_b_hbm, pw2_w_hbm, pw2_b_hbm, scale_hbm]
    weights_here = [norm0_w, norm0_b, down_w, down_b, dw_w, dw_b, norm_w, norm_b, pw1, pw1_b, pw2, pw2_b, layer_scale]
    weight_copies = [pltpu.make_async_copy(far, near, weight_sem.at[n]) for n, (far, near) in enumerate(zip(weights_hbm, weights_here))]
    for copy in weight_copies[:4] + feat_copies[:GI] + weight_copies[4:] + feat_copies[GI:]:
        copy.start()

    barrier = pltpu.get_barrier_semaphore()
    for q in range(8):
        @pl.when(exists(q))
        def _():
            pl.semaphore_signal(barrier, inc=1, device_id=device(q), device_id_type=MESH)

    def zero_rows(first):
        def body(p, _):
            pad[p, pl.ds(first, BORDER)] = jnp.zeros((BORDER, ROW, LANES), F32)
            return 0
        lax.fori_loop(0, pad.shape[0], body, 0)

    def zero_cols(first):
        def body(p, _):
            pad[p, :, pl.ds(first, 8)] = jnp.zeros((pad.shape[1], 8, LANES), F32)
            return 0
        lax.fori_loop(0, pad.shape[0], body, 0)

    pl.when(jnp.logical_not(has_up))(lambda: zero_rows(0))
    pl.when(jnp.logical_not(has_down))(lambda: zero_rows(BORDER + tile_h))
    pl.when(jnp.logical_not(has_left))(lambda: zero_cols(0))
    pl.when(jnp.logical_not(has_right))(lambda: zero_cols(COL0 + tile_w))

    ab[...] = jnp.zeros(ab.shape, BF16)
    row_id = lax.broadcasted_iota(jnp.int32, sel.shape, 0)
    col_id = lax.broadcasted_iota(jnp.int32, sel.shape, 1)
    picked = jnp.where(row_id < tile_h, 2 * row_id, 2 * (row_id - tile_h) + 1)
    sel[...] = jnp.where(col_id == picked, 1.0, 0.0).astype(BF16)
    for copy in weight_copies[:4]:
        copy.wait()
    norm0[0] = jnp.broadcast_to(norm0_w[...].astype(F32), (LANES, ch_in)).T
    norm0[1] = jnp.broadcast_to(norm0_b[...].astype(F32), (LANES, ch_in)).T
    cstage[...] = jnp.zeros(cstage.shape, F32)

    def tail_at(tail, slot):
        rows = tail.shape[0]
        parts = [tail]
        if slot:
            parts = [jnp.zeros((rows, TAIL * slot), tail.dtype)] + parts
        if slot < GI - 1:
            parts = parts + [jnp.zeros((rows, TAIL * (GI - 1 - slot)), tail.dtype)]
        return jnp.concatenate(parts, axis=1)

    for tap in range(4):
        taps = down_w[tap // 2, tap % 2].astype(F32)
        zeros = jnp.zeros((LANES - ch_in, LANES), BF16)
        wd[pl.ds(tap * LANES, ch_in)] = taps[:, :LANES].astype(BF16)
        wd[pl.ds(tap * LANES + ch_in, LANES - ch_in)] = zeros
        for slot in range(GI):
            wdt[slot, pl.ds(tap * LANES, ch_in)] = tail_at(taps[:, LANES:], slot).astype(BF16)
            wdt[slot, pl.ds(tap * LANES + ch_in, LANES - ch_in)] = zeros

    def block_weights():
        for copy in weight_copies[4:]:
            copy.wait()
        for kh in range(7):
            for kw in range(7):
                taps = dw_w[kh, kw].astype(F32)
                tails = jnp.concatenate([taps[:, LANES:]] * GI, axis=1)
                for k in range(2):
                    dwf[k, 0, kh, kw:kw + 1] = taps[k:k + 1, :LANES]
                    dwf[k, 1, kh, kw:kw + 1] = tails[k:k + 1]
        names = [dw_b, norm_w, norm_b, pw2_b, layer_scale]
        for k in range(2):
            for j, ref in enumerate(names):
                head, tail = split(ref[k:k + 1, :])
                vec[k, 0, j:j + 1] = head
                vec[k, 1, j:j + 1] = tail
        for k in range(2):
            w1[k] = (pw1[k, :LANES].astype(F32) * HALF).astype(BF16)
            up_tail = (pw1[k, LANES:].astype(F32) * HALF).astype(BF16)
            for slot in range(GI):
                for other in range(GI):
                    rows = pl.ds(TAIL * other, TAIL)
                    w1t[k, slot, rows] = up_tail if other == slot else jnp.zeros(up_tail.shape, BF16)
                    w2t[k, slot, rows] = pw2[k, LANES:] if other == slot else jnp.zeros(up_tail.shape, BF16)
        lax.fori_loop(0, 7, spread, 0)

    eye[...] = jnp.where(lax.broadcasted_iota(jnp.int32, eye.shape, 0) == lax.broadcasted_iota(jnp.int32, eye.shape, 1), 1.0, 0.0).astype(BF16)

    def spread(kw, _):
        unit = eye[...]
        for k in range(2):
            for kh in range(8):
                if kh < 7:
                    tap = jnp.broadcast_to(dwf[k, 0, kh, pl.ds(kw, 1)], (16, LANES)).astype(BF16)
                    block = unit * jnp.concatenate([tap] * (LANES // 16), axis=0)
                else:
                    block = jnp.zeros((LANES, LANES), BF16)
                diag[k, pl.ds(pl.multiple_of(kw * 4 * LANES, LANES) + kh // 2 * LANES, LANES), kh % 2 * LANES:(kh % 2 + 1) * LANES] = block
        return 0

    pad[:, tile_h + 2 * BORDER:] = jnp.zeros((pad.shape[0], 2, ROW, LANES), F32)

    def split(row):
        row = row.astype(F32)
        return row[:, :LANES], jnp.concatenate([row[:, LANES:]] * GI, axis=1)

    head, tail = split(down_b[...].reshape(1, -1))
    vec[0, 0, 5:6] = head
    vec[0, 1, 5:6] = tail

    flat = pad.reshape(pad.shape[0], pad.shape[1] * ROW, LANES)

    def column(plane, row, col, count):
        return flat.at[plane, pl.ds((BORDER + row) * ROW + COL0 + col, count, stride=ROW), :]

    def messages(k, g):
        base = k * groups * NPL + g * NPL
        planes = pl.ds(base, NPL)
        copies = []
        for q, (dr, dc) in enumerate(steps):
            there = opposite(q)
            if dc == 0:
                first = BORDER if dr < 0 else tile_h
                land = BORDER + tile_h if dr < 0 else 0
                src = pad.at[planes, pl.ds(first, BORDER), pl.ds(COL0, tile_w), :]
                dst = pad.at[planes, pl.ds(land, BORDER), pl.ds(COL0, tile_w), :]
            elif dr == 0:
                src = hsend.at[k, g, q - 2]
                dst = hrecv.at[k, g, there - 2]
            else:
                src = csend.at[k, g, q - 4]
                dst = crecv.at[k, g, there - 4]
            copies.append(pltpu.make_async_remote_copy(
                src_ref=src, dst_ref=dst, send_sem=send_sem.at[k, g, q], recv_sem=recv_sem.at[k, g, there],
                device_id=device(q), device_id_type=MESH))
        return copies

    def send(k, g):
        base = k * groups * NPL + g * NPL
        copies = messages(k, g)
        for q in (2, 3):
            first = 0 if q == 2 else tile_w - BORDER

            for p in range(NPL):
                for j in range(BORDER):
                    hsend[k, g, q - 2, p * BORDER + j] = column(base + p, 0, first + j, tile_h)[...].astype(BF16)
        for q in range(4, 8):
            dr, dc = steps[q]
            first = 0 if dc < 0 else tile_w - BORDER
            row = 0 if dr < 0 else tile_h - BORDER
            for p in range(NPL):
                for j in range(BORDER):
                    cstage[pl.ds((p * BORDER + j) * BORDER, BORDER)] = column(base + p, row, first + j, BORDER)[...]
            csend[k, g, q - 4] = cstage[...].astype(BF16)
        for q in range(8):
            pl.when(exists(q))(copies[q].start)

    def receive(k, g):
        base = k * groups * NPL + g * NPL
        for q in range(8):
            pl.when(exists(q))(_wait_recv(k, g, q))
        for q in (2, 3):
            first = -BORDER if q == 2 else tile_w

            @pl.when(exists(q))
            def _():
                for p in range(NPL):
                    for j in range(BORDER):
                        column(base + p, 0, first + j, tile_h)[...] = hrecv[k, g, q - 2, p * BORDER + j].astype(F32)
        for q in range(4, 8):
            dr, dc = steps[q]
            first = -BORDER if dc < 0 else tile_w
            row = -BORDER if dr < 0 else tile_h

            @pl.when(exists(q))
            def _():
                cstage[...] = crecv[k, g, q - 4].astype(F32)
                for p in range(NPL):
                    for j in range(BORDER):
                        column(base + p, row, first + j, BORDER)[...] = cstage[pl.ds((p * BORDER + j) * BORDER, BORDER)]

    def _wait_recv(k, g, q):
        base = k * groups * NPL + g * NPL
        dr, dc = steps[q]
        if dc == 0:
            land = 0 if dr < 0 else BORDER + tile_h
            dst = pad.at[pl.ds(base, NPL), pl.ds(land, BORDER), pl.ds(COL0, tile_w), :]
        elif dr == 0:
            dst = hrecv.at[k, g, q - 2]
        else:
            dst = crecv.at[k, g, q - 4]

        def wait():
            pltpu.make_async_remote_copy(
                src_ref=dst, dst_ref=dst, send_sem=send_sem.at[k, g, q], recv_sem=recv_sem.at[k, g, q],
                device_id=device(q), device_id_type=MESH).wait_recv()

        return wait

    def wait_send(k, g):
        copies = messages(k, g)
        for q in range(8):
            pl.when(exists(q))(copies[q].wait_send)

    def interior(plane):
        return pad.at[plane, pl.ds(BORDER, tile_h), pl.ds(COL0, tile_w), :]

    def rounded(values):
        return values.astype(BF16).astype(F32)

    def down_norm(g, i, slot):
        img = g * GI + i
        pltpu.make_async_copy(feat.at[img], fv.at[img], feat_sem.at[img]).wait()
        for w in range(in_w):
            x = fv[img, w].astype(F32)
            mean = jnp.sum(x, axis=0, keepdims=True) * (1.0 / ch_in)
            centered = x - mean
            var = jnp.sum(centered * centered, axis=0, keepdims=True) * (1.0 / ch_in)
            a = centered * lax.rsqrt(var + LN_EPS) * norm0[0, :, :in_h] + norm0[1, :, :in_h]
            ab[slot, pl.ds(w * LANES, ch_in), :in_h] = a.astype(BF16)

    def down_conv(g, i, slot):
        turned = lax.dot_general(sel[...], ab[slot], (((1,), (1,)), ((), ())), preferred_element_type=F32).astype(BF16)
        taps = [jnp.concatenate([turned[:tile_h, w * 2 * LANES:(w + 1) * 2 * LANES], turned[tile_h:, w * 2 * LANES:(w + 1) * 2 * LANES]], axis=1) for w in range(tile_w)]
        weights = jnp.concatenate([wd[...], wdt[i]], axis=1)
        d = jnp.dot(jnp.concatenate(taps, axis=0), weights, preferred_element_type=F32)
        head = rounded(d[:, :LANES] + vec[0, 0, 5:6])
        for w in range(tile_w):
            column(g * NPL + i, 0, w, tile_h)[...] = head[w * tile_h:(w + 1) * tile_h]
        ybuf[...] += d[:, LANES:]

    def down_group(g, _):
        ybuf[...] = jnp.zeros(ybuf.shape, F32)

        def two(j, _):
            down_norm(g, 2 * j, 0)
            down_norm(g, 2 * j + 1, 1)
            down_conv(g, 2 * j, 0)
            down_conv(g, 2 * j + 1, 1)
            return 0

        lax.fori_loop(0, GI // 2, two, 0)
        tail = rounded(ybuf[...] + vec[0, 1, 5:6])
        for w in range(tile_w):
            column(g * NPL + GI, 0, w, tile_h)[...] = tail[w * tile_h:(w + 1) * tile_h]

        @pl.when(g == 0)
        def _():
            count = jnp.int32(0)
            for q in range(8):
                count = count + exists(q).astype(jnp.int32)
            pl.semaphore_wait(barrier, count)

        send(0, g)
        return 0

    half = tile_h // 2

    def taps_sum(k, part, plane, r0, count):
        accs = [None] * count
        for kw in range(7):
            xs = [pad[plane, r0 + i, COL0 - BORDER + kw:COL0 - BORDER + kw + 8, :] for i in range(count + 6)]
            for kh in range(7):
                w = jnp.broadcast_to(dwf[k, part, kh, kw:kw + 1, :], (8, LANES))
                for r in range(count):
                    term = xs[r + kh] * w
                    accs[r] = term if accs[r] is None else accs[r] + term
        return accs

    def depthwise(k, g):
        base = k * groups * NPL + g * NPL
        rows2 = (tile_h + 2) * tile_w

        def body(j, _):
            for strip in range(half // 12):
                r0 = j * half + strip * 12
                for r, acc in enumerate(taps_sum(k, 1, base + GI, r0, 12)):
                    ubuf[GI, pl.ds(pl.multiple_of((r0 + r) * 8, 8), 8)] = acc + vec[k, 1, 0:1]
            for strip in range(tile_h // 16):
                for r, acc in enumerate(taps_sum(k, 0, base + 2 + j, strip * 16, 16)):
                    ubuf[2 + j, pl.ds((strip * 16 + r) * 8, 8)] = acc + vec[k, 0, 0:1]

            parts = []
            for kw in range(0,7):
                shifted = pad[base + j, :, COL0 - BORDER + kw:COL0 - BORDER + kw + 8, :].astype(BF16).reshape(-1, LANES)
                for pair in range(4):
                    parts.append(shifted[pair * 16:pair * 16 + rows2])
            sums = jnp.dot(jnp.concatenate(parts, axis=1), diag[k, 0:3584], preferred_element_type=F32)
            part = sums[:pix, :LANES] + sums[8:pix + 8, LANES:]
            ubuf[j] = part + vec[k, 0, 0:1]
            return 0

        lax.fori_loop(0, 2, body, 0)

    LR = 64

    def norm(k):
        nw, nb = vec[k, 0, 1:2], vec[k, 0, 2:3]
        nwt, nbt = vec[k, 1, 1:2], vec[k, 1, 2:3]
        lane = lax.broadcasted_iota(jnp.int32, (LR, LANES), 1)
        channels = LANES + TAIL

        def body(t, _):
            rows = pl.ds(t * LR, LR)
            tail = ubuf[GI, rows]
            heads = [ubuf[i, rows] for i in range(GI)]
            own = [jnp.logical_and(lane >= i * TAIL, lane < (i + 1) * TAIL) for i in range(GI)]

            def pick(cols):
                res = cols[GI - 1]
                for i in range(GI - 2, -1, -1):
                    res = jnp.where(lane < (i + 1) * TAIL, cols[i], res)
                return res

            means = [jnp.sum(heads[i] + jnp.where(own[i], tail, 0.0), axis=-1, keepdims=True) * (1.0 / channels) for i in range(GI)]
            heads = [heads[i] - means[i] for i in range(GI)]
            tail = tail - pick(means)
            square = tail * tail
            rs = [lax.rsqrt(jnp.sum(heads[i] * heads[i] + jnp.where(own[i], square, 0.0), axis=-1, keepdims=True) * (1.0 / channels) + LN_EPS) for i in range(GI)]
            for i in range(GI):
                vbuf[i, rows] = (heads[i] * rs[i] * nw + nb).astype(BF16)
            vbuf[GI, rows] = (tail * pick(rs) * nwt + nbt).astype(BF16)
            return 0

        for t in range(pix // LR):
            body(t, 0)

    def mlp(k, g):
        base = k * groups * NPL + g * NPL
        nxt = groups * NPL + g * NPL
        b1 = pw1_b[k:k + 1, :].astype(F32) * HALF
        def up(i):
            v = jnp.concatenate([vbuf[i], vbuf[GI]], axis=1)
            return jnp.dot(v, jnp.concatenate([w1[k], w1t[k, i]], axis=0), preferred_element_type=F32)

        def act(x):
            x = x + b1
            return (x + x * lax.erf(x * RSQRT2X2)).astype(BF16)

        def down(i, hidden):
            y = lax.dot_general(hidden, jnp.concatenate([pw2[k, :LANES], w2t[k, i]], axis=0), (((1,), (1,)), ((), ())), preferred_element_type=F32)
            head = (y[:, :LANES] + vec[k, 0, 3:4]) * vec[k, 0, 4:5]
            new = interior(base + i)[...] + head.reshape(tile_h, tile_w, LANES)
            if k == 0:
                interior(nxt + i)[...] = rounded(new)
            else:
                obuf[g * GI + i, :, :, :LANES] = new.astype(BF16)
            return y[:, LANES:]

        x = up(0)
        for i in range(GI):
            hidden = act(x)
            if i < GI - 1:
                x = up(i + 1)
            tail = down(i, hidden)
            ybuf[...] = tail if i == 0 else ybuf[...] + tail
        tail = ((ybuf[...] + vec[k, 1, 3:4]) * vec[k, 1, 4:5]).reshape(tile_h, tile_w, LANES)
        new = interior(base + GI)[...] + tail
        if k == 0:
            interior(nxt + GI)[...] = rounded(new)
        else:
            for i in range(GI):
                obuf[g * GI + i, :, :, LANES:] = new[:, :, i * TAIL:(i + 1) * TAIL].astype(BF16)

    def out_copy(g):
        imgs = pl.ds(g * GI, GI)
        return pltpu.make_async_copy(obuf.at[imgs], out.at[imgs], out_sem.at[g])

    def block_group(k):
        def body(g, _):
            receive(k, g)
            depthwise(k, g)
            norm(k)
            mlp(k, g)
            if k == 0:
                send(1, g)
            else:
                out_copy(g).start()
            return 0
        return body

    lax.fori_loop(0, groups, down_group, 0)
    block_weights()
    lax.fori_loop(0, groups, block_group(0), 0)
    lax.fori_loop(0, groups, block_group(1), 0)

    def finish(g, _):
        wait_send(0, g)
        wait_send(1, g)
        out_copy(g).wait()
        return 0

    lax.fori_loop(0, groups, finish, 0)


def solution(mesh):
    rows_count = mesh.shape["sh"]
    cols_count = mesh.shape["sw"]
    act_spec = P("dp", "sh", "sw", None)

    def local_run(feat_map, norm0_w, norm0_b, down_w, down_b, dw_w, dw_b, norm_w, norm_b, pw1_w, pw1_b, pw2_w, pw2_b, layer_scale):
        images, in_h, in_w, ch_in = feat_map.shape
        tile_h, tile_w = in_h // 2, in_w // 2
        ch, hidden = pw1_w.shape[1:]
        groups = images // GI
        pix = tile_h * tile_w
        weights = [
            norm0_w.reshape(1, -1), norm0_b.reshape(1, -1), down_w, down_b, dw_w.transpose(1, 2, 0, 3), dw_b,
            norm_w, norm_b, pw1_w, pw1_b, pw2_w.transpose(0, 2, 1), pw2_b, layer_scale,
        ]
        hbm = pl.BlockSpec(memory_space=pl.ANY)
        return pl.pallas_call(
            functools.partial(kernel, rows_count, cols_count),
            out_shape=jax.ShapeDtypeStruct((images, tile_h, tile_w, ch), BF16),
            in_specs=[hbm] * (1 + len(weights)),
            out_specs=hbm,
            scratch_shapes=[pltpu.VMEM(w.shape, BF16) for w in weights] + [
                pltpu.VMEM((images, in_w, ch_in, in_h), BF16),
                pltpu.VMEM((2, in_w * LANES, LANES), BF16),
                pltpu.VMEM((in_h, LANES), BF16),
                pltpu.VMEM((2, ch_in, LANES), F32),
                pltpu.VMEM((2 * groups * NPL, tile_h + 2 * BORDER + 2, ROW, LANES), F32),
                pltpu.VMEM((2, groups, 2, NPL * BORDER, tile_h, LANES), BF16),
                pltpu.VMEM((2, groups, 2, NPL * BORDER, tile_h, LANES), BF16),
                pltpu.VMEM((2, groups, 4, 48, LANES), BF16),
                pltpu.VMEM((2, groups, 4, 48, LANES), BF16),
                pltpu.VMEM((48, LANES), F32),
                pltpu.VMEM((NPL, pix, LANES), F32),
                pltpu.VMEM((NPL, pix, LANES), BF16),
                pltpu.VMEM((pix, LANES), F32),
                pltpu.VMEM((4 * LANES, LANES), BF16),
                pltpu.VMEM((GI, 4 * LANES, LANES), BF16),
                pltpu.VMEM((2, LANES, hidden), BF16),
                pltpu.VMEM((2, GI, LANES, hidden), BF16),
                pltpu.VMEM((2, GI, LANES, hidden), BF16),
                pltpu.VMEM((2, 2, 7, 8, LANES), F32),
                pltpu.VMEM((LANES, LANES), BF16),
                pltpu.VMEM((2, 7 * 4 * LANES, 2 * LANES), BF16),
                pltpu.VMEM((2, 2, 8, LANES), F32),
                pltpu.VMEM((images, tile_h, tile_w, ch), BF16),
                pltpu.SemaphoreType.DMA((images,)),
                pltpu.SemaphoreType.DMA((len(weights),)),
                pltpu.SemaphoreType.DMA((groups,)),
                pltpu.SemaphoreType.DMA((2, groups, 8)),
                pltpu.SemaphoreType.DMA((2, groups, 8)),
            ],
            compiler_params=pltpu.CompilerParams(collective_id=0, has_side_effects=True, vmem_limit_bytes=63 * 1024 * 1024),
        )(feat_map.transpose(0, 2, 3, 1), *weights)

    return jax.shard_map(local_run, mesh=mesh, in_specs=(act_spec,) + (P(),) * 13, out_specs=act_spec, check_vma=False)
```

```python
import functools

import jax
import jax.numpy as jnp
from jax import lax
from jax.experimental import pallas as pl
from jax.experimental.pallas import tpu as pltpu
from jax.sharding import PartitionSpec as P

LN_EPS = 1e-6
MESH = pl.DeviceIdType.MESH
GI = 4
NPL = GI + 1
LANES = 128
TAIL = 32
ROW = 24
COL0 = 8
BORDER = 3
HALF = 0.5
RSQRT2X2 = 1.4142135623730951

F32 = jnp.float32
BF16 = jnp.bfloat16


def kernel(
    rows_count, cols_count,
    feat, norm0_w_hbm, norm0_b_hbm, down_w_hbm, down_b_hbm, dw_w_hbm, dw_b_hbm, norm_w_hbm, norm_b_hbm, pw1_w_hbm, pw1_b_hbm, pw2_w_hbm, pw2_b_hbm, scale_hbm,
    out,
    norm0_w, norm0_b, down_w, down_b, dw_w, dw_b, norm_w, norm_b, pw1, pw1_b, pw2, pw2_b, layer_scale,
    fv, ab, sel, norm0, pad, hsend, hrecv, csend, crecv, cstage, ubuf, vbuf, ybuf, wd, wdt, w1, w1t, w2t, dwf, eye, diag, vec, obuf,
    feat_sem, weight_sem, out_sem, send_sem, recv_sem,
):
    images, in_w, ch_in, in_h = fv.shape
    groups = images // GI
    tile_h, tile_w = obuf.shape[1], obuf.shape[2]
    pix = tile_h * tile_w
    my_row, my_col = lax.axis_index("sh"), lax.axis_index("sw")
    has_up, has_down = my_row > 0, my_row < rows_count - 1
    has_left, has_right = my_col > 0, my_col < cols_count - 1

    steps = [(-1, 0), (1, 0), (0, -1), (0, 1), (-1, -1), (-1, 1), (1, -1), (1, 1)]
    steps += [(0, -1), (0, 1)]
    row_ok = {-1: has_up, 0: None, 1: has_down}
    col_ok = {-1: has_left, 0: None, 1: has_right}

    def exists(q):
        dr, dc = steps[q]
        if row_ok[dr] is None:
            return col_ok[dc]
        if col_ok[dc] is None:
            return row_ok[dr]
        return jnp.logical_and(row_ok[dr], col_ok[dc])

    def opposite(q):
        dr, dc = steps[q]
        return q ^ 1 if dr == 0 else steps.index((-dr, -dc))

    def device(q):
        dr, dc = steps[q]
        return {"sh": my_row + dr, "sw": my_col + dc}

    feat_copies = [pltpu.make_async_copy(feat.at[i], fv.at[i], feat_sem.at[i]) for i in range(images)]
    weights_hbm = [norm0_w_hbm, norm0_b_hbm, down_w_hbm, down_b_hbm, dw_w_hbm, dw_b_hbm, norm_w_hbm, norm_b_hbm, pw1_w_hbm, pw1_b_hbm, pw2_w_hbm, pw2_b_hbm, scale_hbm]
    weights_here = [norm0_w, norm0_b, down_w, down_b, dw_w, dw_b, norm_w, norm_b, pw1, pw1_b, pw2, pw2_b, layer_scale]
    weight_copies = [pltpu.make_async_copy(far, near, weight_sem.at[n]) for n, (far, near) in enumerate(zip(weights_hbm, weights_here))]
    for copy in weight_copies[:4] + feat_copies[:GI] + weight_copies[4:] + feat_copies[GI:]:
        copy.start()

    barrier = pltpu.get_barrier_semaphore()
    for q in range(8):
        @pl.when(exists(q))
        def _():
            pl.semaphore_signal(barrier, inc=1, device_id=device(q), device_id_type=MESH)

    def zero_rows(first):
        def body(p, _):
            pad[p, pl.ds(first, BORDER)] = jnp.zeros((BORDER, ROW, LANES), F32)
            return 0
        lax.fori_loop(0, pad.shape[0], body, 0)

    def zero_cols(first):
        def body(p, _):
            pad[p, :, pl.ds(first, 8)] = jnp.zeros((pad.shape[1], 8, LANES), F32)
            return 0
        lax.fori_loop(0, pad.shape[0], body, 0)

    pl.when(jnp.logical_not(has_up))(lambda: zero_rows(0))
    pl.when(jnp.logical_not(has_down))(lambda: zero_rows(BORDER + tile_h))
    pl.when(jnp.logical_not(has_left))(lambda: zero_cols(0))
    pl.when(jnp.logical_not(has_right))(lambda: zero_cols(COL0 + tile_w))

    ab[...] = jnp.zeros(ab.shape, BF16)
    row_id = lax.broadcasted_iota(jnp.int32, sel.shape, 0)
    col_id = lax.broadcasted_iota(jnp.int32, sel.shape, 1)
    picked = jnp.where(row_id < tile_h, 2 * row_id, 2 * (row_id - tile_h) + 1)
    sel[...] = jnp.where(col_id == picked, 1.0, 0.0).astype(BF16)
    for copy in weight_copies[:4]:
        copy.wait()
    norm0[0] = jnp.broadcast_to(norm0_w[...].astype(F32), (LANES, ch_in)).T
    norm0[1] = jnp.broadcast_to(norm0_b[...].astype(F32), (LANES, ch_in)).T
    cstage[...] = jnp.zeros(cstage.shape, F32)

    def tail_at(tail, slot):
        rows = tail.shape[0]
        parts = [tail]
        if slot:
            parts = [jnp.zeros((rows, TAIL * slot), tail.dtype)] + parts
        if slot < GI - 1:
            parts = parts + [jnp.zeros((rows, TAIL * (GI - 1 - slot)), tail.dtype)]
        return jnp.concatenate(parts, axis=1)

    for kh in range(2):
        zeros = jnp.zeros((2 * LANES - 2 * ch_in, LANES), BF16)
        wd[pl.ds(kh * 2 * LANES + 2 * ch_in, 2 * LANES - 2 * ch_in)] = zeros
        for kw in range(2):
            taps = down_w[kh, kw].astype(F32)
            rows = pl.ds(kh * 2 * LANES + kw * ch_in, ch_in)
            wd[rows] = taps[:, :LANES].astype(BF16)
            for slot in range(GI):
                wdt[slot, rows] = tail_at(taps[:, LANES:], slot).astype(BF16)
        for slot in range(GI):
            wdt[slot, pl.ds(kh * 2 * LANES + 2 * ch_in, 2 * LANES - 2 * ch_in)] = zeros

    def block_weights():
        for copy in weight_copies[4:]:
            copy.wait()
        for kh in range(7):
            for kw in range(7):
                taps = dw_w[kh, kw].astype(F32)
                tails = jnp.concatenate([taps[:, LANES:]] * GI, axis=1)
                for k in range(2):
                    dwf[k, 0, kh, kw:kw + 1] = taps[k:k + 1, :LANES]
                    dwf[k, 1, kh, kw:kw + 1] = tails[k:k + 1]
        names = [dw_b, norm_w, norm_b, pw2_b, layer_scale]
        for k in range(2):
            for j, ref in enumerate(names):
                head, tail = split(ref[k:k + 1, :])
                vec[k, 0, j:j + 1] = head
                vec[k, 1, j:j + 1] = tail
        for k in range(2):
            w1[k] = (pw1[k, :LANES].astype(F32) * HALF).astype(BF16)
            up_tail = (pw1[k, LANES:].astype(F32) * HALF).astype(BF16)
            for slot in range(GI):
                for other in range(GI):
                    rows = pl.ds(TAIL * other, TAIL)
                    w1t[k, slot, rows] = up_tail if other == slot else jnp.zeros(up_tail.shape, BF16)
                    w2t[k, slot, rows] = pw2[k, LANES:] if other == slot else jnp.zeros(up_tail.shape, BF16)
        lax.fori_loop(0, 7, spread, 0)

    eye[...] = jnp.where(lax.broadcasted_iota(jnp.int32, eye.shape, 0) == lax.broadcasted_iota(jnp.int32, eye.shape, 1), 1.0, 0.0).astype(BF16)

    def spread(kw, _):
        unit = eye[...]
        for k in range(2):
            for kh in range(8):
                if kh < 7:
                    tap = jnp.broadcast_to(dwf[k, 0, kh, pl.ds(kw, 1)], (16, LANES)).astype(BF16)
                    block = unit * jnp.concatenate([tap] * (LANES // 16), axis=0)
                else:
                    block = jnp.zeros((LANES, LANES), BF16)
                diag[k, pl.ds(pl.multiple_of(kw * 4 * LANES, LANES) + kh // 2 * LANES, LANES), kh % 2 * LANES:(kh % 2 + 1) * LANES] = block
        return 0

    pad[:, tile_h + 2 * BORDER:] = jnp.zeros((pad.shape[0], 2, ROW, LANES), F32)

    def split(row):
        row = row.astype(F32)
        return row[:, :LANES], jnp.concatenate([row[:, LANES:]] * GI, axis=1)

    head, tail = split(down_b[...].reshape(1, -1))
    vec[0, 0, 5:6] = head
    vec[0, 1, 5:6] = tail

    flat = pad.reshape(pad.shape[0], pad.shape[1] * ROW, LANES)

    def column(plane, row, col, count):
        return flat.at[plane, pl.ds((BORDER + row) * ROW + COL0 + col, count, stride=ROW), :]

    def side_rows(q):
        return pl.ds(0, 2 * BORDER) if q >= 8 else pl.ds(2 * BORDER, (NPL - 2) * BORDER)

    def messages(k, g):
        base = k * groups * NPL + g * NPL
        planes = pl.ds(base, NPL)
        copies = []
        for q, (dr, dc) in enumerate(steps):
            there = opposite(q)
            if dc == 0:
                first = BORDER if dr < 0 else tile_h
                land = BORDER + tile_h if dr < 0 else 0
                src = pad.at[planes, pl.ds(first, BORDER), pl.ds(COL0, tile_w), :]
                dst = pad.at[planes, pl.ds(land, BORDER), pl.ds(COL0, tile_w), :]
            elif dr == 0:
                src = hsend.at[k, g, q % 2, side_rows(q)]
                dst = hrecv.at[k, g, there % 2, side_rows(q)]
            else:
                src = csend.at[k, g, q - 4]
                dst = crecv.at[k, g, there - 4]
            copies.append(pltpu.make_async_remote_copy(
                src_ref=src, dst_ref=dst, send_sem=send_sem.at[k, g, q], recv_sem=recv_sem.at[k, g, there],
                device_id=device(q), device_id_type=MESH))
        return copies

    def fill_sides(k, g, planes):
        base = k * groups * NPL + g * NPL
        for side, first in ((0, 0), (1, tile_w - BORDER)):
            for p in planes:
                for j in range(BORDER):
                    hsend[k, g, side, p * BORDER + j] = column(base + p, 0, first + j, tile_h)[...].astype(BF16)

    def send_early(k, g):
        copies = messages(k, g)
        fill_sides(k, g, range(2))
        for q in (8, 9):
            pl.when(exists(q))(copies[q].start)

    def send_late(k, g):
        base = k * groups * NPL + g * NPL
        copies = messages(k, g)
        fill_sides(k, g, range(2, NPL))
        for q in range(4, 8):
            dr, dc = steps[q]
            first = 0 if dc < 0 else tile_w - BORDER
            row = 0 if dr < 0 else tile_h - BORDER
            for p in range(NPL):
                for j in range(BORDER):
                    cstage[pl.ds((p * BORDER + j) * BORDER, BORDER)] = column(base + p, row, first + j, BORDER)[...]
            csend[k, g, q - 4] = cstage[...].astype(BF16)
        for q in (2, 3, 4, 5, 6, 7, 0, 1):
            pl.when(exists(q))(copies[q].start)

    def receive(k, g):
        base = k * groups * NPL + g * NPL
        for q in range(len(steps)):
            pl.when(exists(q))(_wait_recv(k, g, q))
        for q in (2, 3):
            first = -BORDER if q == 2 else tile_w

            @pl.when(exists(q))
            def _():
                for p in range(NPL):
                    for j in range(BORDER):
                        column(base + p, 0, first + j, tile_h)[...] = hrecv[k, g, q - 2, p * BORDER + j].astype(F32)
        for q in range(4, 8):
            dr, dc = steps[q]
            first = -BORDER if dc < 0 else tile_w
            row = -BORDER if dr < 0 else tile_h

            @pl.when(exists(q))
            def _():
                cstage[...] = crecv[k, g, q - 4].astype(F32)
                for p in range(NPL):
                    for j in range(BORDER):
                        column(base + p, row, first + j, BORDER)[...] = cstage[pl.ds((p * BORDER + j) * BORDER, BORDER)]

    def _wait_recv(k, g, q):
        base = k * groups * NPL + g * NPL
        dr, dc = steps[q]
        if dc == 0:
            land = 0 if dr < 0 else BORDER + tile_h
            dst = pad.at[pl.ds(base, NPL), pl.ds(land, BORDER), pl.ds(COL0, tile_w), :]
        elif dr == 0:
            dst = hrecv.at[k, g, q % 2, side_rows(q)]
        else:
            dst = crecv.at[k, g, q - 4]

        def wait():
            pltpu.make_async_remote_copy(
                src_ref=dst, dst_ref=dst, send_sem=send_sem.at[k, g, q], recv_sem=recv_sem.at[k, g, q],
                device_id=device(q), device_id_type=MESH).wait_recv()

        return wait

    def wait_send(k, g):
        copies = messages(k, g)
        for q in range(len(steps)):
            pl.when(exists(q))(copies[q].wait_send)

    def interior(plane):
        return pad.at[plane, pl.ds(BORDER, tile_h), pl.ds(COL0, tile_w), :]

    def rounded(values):
        return values.astype(BF16).astype(F32)

    def down_norm(g, i, slot):
        img = g * GI + i
        pltpu.make_async_copy(feat.at[img], fv.at[img], feat_sem.at[img]).wait()
        for w in range(in_w):
            x = fv[img, w].astype(F32)
            mean = jnp.sum(x, axis=0, keepdims=True) * (1.0 / ch_in)
            centered = x - mean
            var = jnp.sum(centered * centered, axis=0, keepdims=True) * (1.0 / ch_in)
            a = centered * lax.rsqrt(var + LN_EPS) * norm0[0, :, :in_h] + norm0[1, :, :in_h]
            ab[slot, pl.ds(w * ch_in, ch_in), :in_h] = a.astype(BF16)

    def down_conv(g, i, slot):
        turned = lax.dot_general(sel[...], ab[slot], (((1,), (1,)), ((), ())), preferred_element_type=F32).astype(BF16)
        pair = 2 * ch_in
        taps = []
        for w in range(tile_w):
            window = turned[:, w * pair:min(w * pair + 2 * LANES, turned.shape[1])]
            if window.shape[1] < 2 * LANES:
                window = jnp.concatenate([window, jnp.zeros((in_h, 2 * LANES - window.shape[1]), BF16)], axis=1)
            taps.append(jnp.concatenate([window[:tile_h], window[tile_h:]], axis=1))
        weights = jnp.concatenate([wd[...], wdt[i]], axis=1)
        d = jnp.dot(jnp.concatenate(taps, axis=0), weights, preferred_element_type=F32)
        head = rounded(d[:, :LANES] + vec[0, 0, 5:6])
        for w in range(tile_w):
            column(g * NPL + i, 0, w, tile_h)[...] = head[w * tile_h:(w + 1) * tile_h]
        ybuf[...] += d[:, LANES:]

    def down_group(g, _):
        ybuf[...] = jnp.zeros(ybuf.shape, F32)

        def two(j):
            down_norm(g, 2 * j, 0)
            down_norm(g, 2 * j + 1, 1)
            down_conv(g, 2 * j, 0)
            down_conv(g, 2 * j + 1, 1)

        two(0)

        @pl.when(g == 0)
        def _():
            count = jnp.int32(0)
            for q in range(8):
                count = count + exists(q).astype(jnp.int32)
            pl.semaphore_wait(barrier, count)

        send_early(0, g)
        two(1)
        tail = rounded(ybuf[...] + vec[0, 1, 5:6])
        for w in range(tile_w):
            column(g * NPL + GI, 0, w, tile_h)[...] = tail[w * tile_h:(w + 1) * tile_h]
        send_late(0, g)
        return 0

    half = tile_h // 2

    def taps_sum(k, part, plane, r0, count):
        accs = [None] * count
        for kw in range(7):
            xs = [pad[plane, r0 + i, COL0 - BORDER + kw:COL0 - BORDER + kw + 8, :] for i in range(count + 6)]
            for kh in range(7):
                w = jnp.broadcast_to(dwf[k, part, kh, kw:kw + 1, :], (8, LANES))
                for r in range(count):
                    term = xs[r + kh] * w
                    accs[r] = term if accs[r] is None else accs[r] + term
        return accs

    def depthwise(k, g):
        base = k * groups * NPL + g * NPL
        rows2 = (tile_h + 2) * tile_w

        def body(j, _):
            for strip in range(half // 12):
                r0 = j * half + strip * 12
                for r, acc in enumerate(taps_sum(k, 1, base + GI, r0, 12)):
                    ubuf[GI, pl.ds(pl.multiple_of((r0 + r) * 8, 8), 8)] = acc + vec[k, 1, 0:1]
            for strip in range(tile_h // 16):
                for r, acc in enumerate(taps_sum(k, 0, base + 2 + j, strip * 16, 16)):
                    ubuf[2 + j, pl.ds((strip * 16 + r) * 8, 8)] = acc + vec[k, 0, 0:1]

            parts = []
            for kw in range(0,7):
                shifted = pad[base + j, :, COL0 - BORDER + kw:COL0 - BORDER + kw + 8, :].astype(BF16).reshape(-1, LANES)
                for pair in range(4):
                    parts.append(shifted[pair * 16:pair * 16 + rows2])
            sums = jnp.dot(jnp.concatenate(parts, axis=1), diag[k, 0:3584], preferred_element_type=F32)
            part = sums[:pix, :LANES] + sums[8:pix + 8, LANES:]
            ubuf[j] = part + vec[k, 0, 0:1]
            return 0

        lax.fori_loop(0, 2, body, 0)

    LR = 64

    def norm(k):
        nw, nb = vec[k, 0, 1:2], vec[k, 0, 2:3]
        nwt, nbt = vec[k, 1, 1:2], vec[k, 1, 2:3]
        lane = lax.broadcasted_iota(jnp.int32, (LR, LANES), 1)
        channels = LANES + TAIL

        def body(t, _):
            rows = pl.ds(t * LR, LR)
            tail = ubuf[GI, rows]
            heads = [ubuf[i, rows] for i in range(GI)]
            own = [jnp.logical_and(lane >= i * TAIL, lane < (i + 1) * TAIL) for i in range(GI)]

            def pick(cols):
                res = cols[GI - 1]
                for i in range(GI - 2, -1, -1):
                    res = jnp.where(lane < (i + 1) * TAIL, cols[i], res)
                return res

            means = [jnp.sum(heads[i] + jnp.where(own[i], tail, 0.0), axis=-1, keepdims=True) * (1.0 / channels) for i in range(GI)]
            heads = [heads[i] - means[i] for i in range(GI)]
            tail = tail - pick(means)
            square = tail * tail
            rs = [lax.rsqrt(jnp.sum(heads[i] * heads[i] + jnp.where(own[i], square, 0.0), axis=-1, keepdims=True) * (1.0 / channels) + LN_EPS) for i in range(GI)]
            for i in range(GI):
                vbuf[i, rows] = (heads[i] * rs[i] * nw + nb).astype(BF16)
            vbuf[GI, rows] = (tail * pick(rs) * nwt + nbt).astype(BF16)
            return 0

        for t in range(pix // LR):
            body(t, 0)

    def mlp(k, g):
        base = k * groups * NPL + g * NPL
        nxt = groups * NPL + g * NPL
        b1 = pw1_b[k:k + 1, :].astype(F32) * HALF
        def up(i):
            v = jnp.concatenate([vbuf[i], vbuf[GI]], axis=1)
            return jnp.dot(v, jnp.concatenate([w1[k], w1t[k, i]], axis=0), preferred_element_type=F32)

        def act(x):
            x = x + b1
            return (x + x * lax.erf(x * RSQRT2X2)).astype(BF16)

        def down(i, hidden):
            y = lax.dot_general(hidden, jnp.concatenate([pw2[k, :LANES], w2t[k, i]], axis=0), (((1,), (1,)), ((), ())), preferred_element_type=F32)
            head = (y[:, :LANES] + vec[k, 0, 3:4]) * vec[k, 0, 4:5]
            new = interior(base + i)[...] + head.reshape(tile_h, tile_w, LANES)
            if k == 0:
                interior(nxt + i)[...] = rounded(new)
            else:
                obuf[g * GI + i, :, :, :LANES] = new.astype(BF16)
            return y[:, LANES:]

        x = up(0)
        for i in range(GI):
            hidden = act(x)
            if i < GI - 1:
                x = up(i + 1)
            tail = down(i, hidden)
            ybuf[...] = tail if i == 0 else ybuf[...] + tail
        tail = ((ybuf[...] + vec[k, 1, 3:4]) * vec[k, 1, 4:5]).reshape(tile_h, tile_w, LANES)
        new = interior(base + GI)[...] + tail
        if k == 0:
            interior(nxt + GI)[...] = rounded(new)
        else:
            for i in range(GI):
                obuf[g * GI + i, :, :, LANES:] = new[:, :, i * TAIL:(i + 1) * TAIL].astype(BF16)

    def out_copy(g):
        imgs = pl.ds(g * GI, GI)
        return pltpu.make_async_copy(obuf.at[imgs], out.at[imgs], out_sem.at[g])

    def block_group(k):
        def body(g, _):
            receive(k, g)
            depthwise(k, g)
            norm(k)
            mlp(k, g)
            if k == 0:
                send_early(1, g)
                send_late(1, g)
            else:
                out_copy(g).start()
            return 0
        return body

    lax.fori_loop(0, groups, down_group, 0)
    block_weights()
    lax.fori_loop(0, groups, block_group(0), 0)
    lax.fori_loop(0, groups, block_group(1), 0)

    def finish(g, _):
        wait_send(0, g)
        wait_send(1, g)
        out_copy(g).wait()
        return 0

    lax.fori_loop(0, groups, finish, 0)


def solution(mesh):
    rows_count = mesh.shape["sh"]
    cols_count = mesh.shape["sw"]
    act_spec = P("dp", "sh", "sw", None)

    def local_run(feat_map, norm0_w, norm0_b, down_w, down_b, dw_w, dw_b, norm_w, norm_b, pw1_w, pw1_b, pw2_w, pw2_b, layer_scale):
        images, in_h, in_w, ch_in = feat_map.shape
        tile_h, tile_w = in_h // 2, in_w // 2
        ch, hidden = pw1_w.shape[1:]
        groups = images // GI
        pix = tile_h * tile_w
        weights = [
            norm0_w.reshape(1, -1), norm0_b.reshape(1, -1), down_w, down_b, dw_w.transpose(1, 2, 0, 3), dw_b,
            norm_w, norm_b, pw1_w, pw1_b, pw2_w.transpose(0, 2, 1), pw2_b, layer_scale,
        ]
        hbm = pl.BlockSpec(memory_space=pl.ANY)
        return pl.pallas_call(
            functools.partial(kernel, rows_count, cols_count),
            out_shape=jax.ShapeDtypeStruct((images, tile_h, tile_w, ch), BF16),
            in_specs=[hbm] * (1 + len(weights)),
            out_specs=hbm,
            scratch_shapes=[pltpu.VMEM(w.shape, BF16) for w in weights] + [
                pltpu.VMEM((images, in_w, ch_in, in_h), BF16),
                pltpu.VMEM((2, in_w * ch_in, LANES), BF16),
                pltpu.VMEM((in_h, LANES), BF16),
                pltpu.VMEM((2, ch_in, LANES), F32),
                pltpu.VMEM((2 * groups * NPL, tile_h + 2 * BORDER + 2, ROW, LANES), F32),
                pltpu.VMEM((2, groups, 2, NPL * BORDER, tile_h, LANES), BF16),
                pltpu.VMEM((2, groups, 2, NPL * BORDER, tile_h, LANES), BF16),
                pltpu.VMEM((2, groups, 4, 48, LANES), BF16),
                pltpu.VMEM((2, groups, 4, 48, LANES), BF16),
                pltpu.VMEM((48, LANES), F32),
                pltpu.VMEM((NPL, pix, LANES), F32),
                pltpu.VMEM((NPL, pix, LANES), BF16),
                pltpu.VMEM((pix, LANES), F32),
                pltpu.VMEM((4 * LANES, LANES), BF16),
                pltpu.VMEM((GI, 4 * LANES, LANES), BF16),
                pltpu.VMEM((2, LANES, hidden), BF16),
                pltpu.VMEM((2, GI, LANES, hidden), BF16),
                pltpu.VMEM((2, GI, LANES, hidden), BF16),
                pltpu.VMEM((2, 2, 7, 8, LANES), F32),
                pltpu.VMEM((LANES, LANES), BF16),
                pltpu.VMEM((2, 7 * 4 * LANES, 2 * LANES), BF16),
                pltpu.VMEM((2, 2, 8, LANES), F32),
                pltpu.VMEM((images, tile_h, tile_w, ch), BF16),
                pltpu.SemaphoreType.DMA((images,)),
                pltpu.SemaphoreType.DMA((len(weights),)),
                pltpu.SemaphoreType.DMA((groups,)),
                pltpu.SemaphoreType.DMA((2, groups, 10)),
                pltpu.SemaphoreType.DMA((2, groups, 10)),
            ],
            compiler_params=pltpu.CompilerParams(collective_id=0, has_side_effects=True, vmem_limit_bytes=63 * 1024 * 1024),
        )(feat_map.transpose(0, 2, 3, 1), *weights)

    return jax.shard_map(local_run, mesh=mesh, in_specs=(act_spec,) + (P(),) * 13, out_specs=act_spec, check_vma=False)
```

```python
import functools

import jax
import jax.numpy as jnp
from jax import lax
from jax.experimental import pallas as pl
from jax.experimental.pallas import tpu as pltpu
from jax.sharding import PartitionSpec as P

LN_EPS = 1e-6
MESH = pl.DeviceIdType.MESH
GI = 4
NPL = GI + 1
LANES = 128
TAIL = 32
ROW = 24
COL0 = 8
BORDER = 3
HALF = 0.5
RSQRT2X2 = 1.4142135623730951

F32 = jnp.float32
BF16 = jnp.bfloat16


def kernel(
    rows_count, cols_count,
    feat, norm0_w_hbm, norm0_b_hbm, down_w_hbm, down_b_hbm, dw_w_hbm, dw_b_hbm, norm_w_hbm, norm_b_hbm, pw1_w_hbm, pw1_b_hbm, pw2_w_hbm, pw2_b_hbm, scale_hbm,
    out,
    norm0_w, norm0_b, down_w, down_b, dw_w, dw_b, norm_w, norm_b, pw1, pw1_b, pw2, pw2_b, layer_scale,
    fv, ab, sel, norm0, pad, hsend, hrecv, csend, crecv, cstage, ubuf, vbuf, ybuf, wd, wdt, w1, w1t, w2t, dwf, eye, diag, vec, obuf,
    feat_sem, weight_sem, out_sem, send_sem, recv_sem,
):
    images, in_w, ch_in, in_h = fv.shape
    groups = images // GI
    tile_h, tile_w = obuf.shape[1], obuf.shape[2]
    pix = tile_h * tile_w
    my_row, my_col = lax.axis_index("sh"), lax.axis_index("sw")
    has_up, has_down = my_row > 0, my_row < rows_count - 1
    has_left, has_right = my_col > 0, my_col < cols_count - 1

    steps = [(-1, 0), (1, 0), (0, -1), (0, 1), (-1, -1), (-1, 1), (1, -1), (1, 1)]
    steps += [(0, -1), (0, 1)]
    row_ok = {-1: has_up, 0: None, 1: has_down}
    col_ok = {-1: has_left, 0: None, 1: has_right}

    def exists(q):
        dr, dc = steps[q]
        if row_ok[dr] is None:
            return col_ok[dc]
        if col_ok[dc] is None:
            return row_ok[dr]
        return jnp.logical_and(row_ok[dr], col_ok[dc])

    def opposite(q):
        dr, dc = steps[q]
        return q ^ 1 if dr == 0 else steps.index((-dr, -dc))

    def device(q):
        dr, dc = steps[q]
        return {"sh": my_row + dr, "sw": my_col + dc}

    feat_copies = [pltpu.make_async_copy(feat.at[i], fv.at[i], feat_sem.at[i]) for i in range(images)]
    weights_hbm = [norm0_w_hbm, norm0_b_hbm, down_w_hbm, down_b_hbm, dw_w_hbm, dw_b_hbm, norm_w_hbm, norm_b_hbm, pw1_w_hbm, pw1_b_hbm, pw2_w_hbm, pw2_b_hbm, scale_hbm]
    weights_here = [norm0_w, norm0_b, down_w, down_b, dw_w, dw_b, norm_w, norm_b, pw1, pw1_b, pw2, pw2_b, layer_scale]
    weight_copies = [pltpu.make_async_copy(far, near, weight_sem.at[n]) for n, (far, near) in enumerate(zip(weights_hbm, weights_here))]
    for copy in weight_copies[:4] + feat_copies[:GI]:
        copy.start()

    barrier = pltpu.get_barrier_semaphore()
    for q in range(8):
        @pl.when(exists(q))
        def _():
            pl.semaphore_signal(barrier, inc=1, device_id=device(q), device_id_type=MESH)

    def zero_rows(first):
        def body(p, _):
            pad[p, pl.ds(first, BORDER)] = jnp.zeros((BORDER, ROW, LANES), F32)
            return 0
        lax.fori_loop(0, pad.shape[0], body, 0)

    def zero_cols(first):
        def body(p, _):
            pad[p, :, pl.ds(first, 8)] = jnp.zeros((pad.shape[1], 8, LANES), F32)
            return 0
        lax.fori_loop(0, pad.shape[0], body, 0)

    pl.when(jnp.logical_not(has_up))(lambda: zero_rows(0))
    pl.when(jnp.logical_not(has_down))(lambda: zero_rows(BORDER + tile_h))
    pl.when(jnp.logical_not(has_left))(lambda: zero_cols(0))
    pl.when(jnp.logical_not(has_right))(lambda: zero_cols(COL0 + tile_w))

    ab[...] = jnp.zeros(ab.shape, BF16)
    row_id = lax.broadcasted_iota(jnp.int32, sel.shape, 0)
    col_id = lax.broadcasted_iota(jnp.int32, sel.shape, 1)
    picked = jnp.where(row_id < tile_h, 2 * row_id, 2 * (row_id - tile_h) + 1)
    sel[...] = jnp.where(col_id == picked, 1.0, 0.0).astype(BF16)
    for copy in weight_copies[:4]:
        copy.wait()
    norm0[0] = jnp.broadcast_to(norm0_w[...].astype(F32), (LANES, ch_in)).T
    norm0[1] = jnp.broadcast_to(norm0_b[...].astype(F32), (LANES, ch_in)).T
    cstage[...] = jnp.zeros(cstage.shape, F32)

    def tail_at(tail, slot):
        rows = tail.shape[0]
        parts = [tail]
        if slot:
            parts = [jnp.zeros((rows, TAIL * slot), tail.dtype)] + parts
        if slot < GI - 1:
            parts = parts + [jnp.zeros((rows, TAIL * (GI - 1 - slot)), tail.dtype)]
        return jnp.concatenate(parts, axis=1)

    for kh in range(2):
        zeros = jnp.zeros((2 * LANES - 2 * ch_in, LANES), BF16)
        wd[pl.ds(kh * 2 * LANES + 2 * ch_in, 2 * LANES - 2 * ch_in)] = zeros
        for kw in range(2):
            taps = down_w[kh, kw].astype(F32)
            rows = pl.ds(kh * 2 * LANES + kw * ch_in, ch_in)
            wd[rows] = taps[:, :LANES].astype(BF16)
            for slot in range(GI):
                wdt[slot, rows] = tail_at(taps[:, LANES:], slot).astype(BF16)
        for slot in range(GI):
            wdt[slot, pl.ds(kh * 2 * LANES + 2 * ch_in, 2 * LANES - 2 * ch_in)] = zeros

    def block_weights():
        for copy in weight_copies[4:]:
            copy.wait()
        for kh in range(7):
            for kw in range(7):
                taps = dw_w[kh, kw].astype(F32)
                tails = jnp.concatenate([taps[:, LANES:]] * GI, axis=1)
                for k in range(2):
                    dwf[k, 0, kh, kw:kw + 1] = taps[k:k + 1, :LANES]
                    dwf[k, 1, kh, kw:kw + 1] = tails[k:k + 1]
        names = [dw_b, norm_w, norm_b, pw2_b, layer_scale]
        for k in range(2):
            for j, ref in enumerate(names):
                head, tail = split(ref[k:k + 1, :])
                vec[k, 0, j:j + 1] = head
                vec[k, 1, j:j + 1] = tail
        for k in range(2):
            w1[k] = (pw1[k, :LANES].astype(F32) * HALF).astype(BF16)
            up_tail = (pw1[k, LANES:].astype(F32) * HALF).astype(BF16)
            for slot in range(GI):
                for other in range(GI):
                    rows = pl.ds(TAIL * other, TAIL)
                    w1t[k, slot, rows] = up_tail if other == slot else jnp.zeros(up_tail.shape, BF16)
                    w2t[k, slot, rows] = pw2[k, LANES:] if other == slot else jnp.zeros(up_tail.shape, BF16)
        for kw in range(7):
            spread(kw, 0)

    eye[...] = jnp.where(lax.broadcasted_iota(jnp.int32, eye.shape, 0) == lax.broadcasted_iota(jnp.int32, eye.shape, 1), 1.0, 0.0).astype(BF16)

    def spread(kw, _):
        unit = eye[...]
        for k in range(2):
            for kh in range(8):
                if kh < 7:
                    tap = jnp.broadcast_to(dwf[k, 0, kh, kw:kw + 1], (16, LANES)).astype(BF16)
                    block = unit * jnp.concatenate([tap] * (LANES // 16), axis=0)
                else:
                    block = jnp.zeros((LANES, LANES), BF16)
                diag[k, pl.ds((kw * 4 + kh // 2) * LANES, LANES), kh % 2 * LANES:(kh % 2 + 1) * LANES] = block
        return 0

    pad[:, tile_h + 2 * BORDER:] = jnp.zeros((pad.shape[0], 2, ROW, LANES), F32)

    def split(row):
        row = row.astype(F32)
        return row[:, :LANES], jnp.concatenate([row[:, LANES:]] * GI, axis=1)

    head, tail = split(down_b[...].reshape(1, -1))
    vec[0, 0, 5:6] = head
    vec[0, 1, 5:6] = tail

    flat = pad.reshape(pad.shape[0], pad.shape[1] * ROW, LANES)

    def column(plane, row, col, count):
        return flat.at[plane, pl.ds((BORDER + row) * ROW + COL0 + col, count, stride=ROW), :]

    def side_rows(q):
        return pl.ds(0, 2 * BORDER) if q >= 8 else pl.ds(2 * BORDER, (NPL - 2) * BORDER)

    def messages(k, g):
        base = k * groups * NPL + g * NPL
        planes = pl.ds(base, NPL)
        copies = []
        for q, (dr, dc) in enumerate(steps):
            there = opposite(q)
            if dc == 0:
                first = BORDER if dr < 0 else tile_h
                land = BORDER + tile_h if dr < 0 else 0
                src = pad.at[planes, pl.ds(first, BORDER), pl.ds(COL0, tile_w), :]
                dst = pad.at[planes, pl.ds(land, BORDER), pl.ds(COL0, tile_w), :]
            elif dr == 0:
                src = hsend.at[k, g, q % 2, side_rows(q)]
                dst = hrecv.at[k, g, there % 2, side_rows(q)]
            else:
                src = csend.at[k, g, q - 4]
                dst = crecv.at[k, g, there - 4]
            copies.append(pltpu.make_async_remote_copy(
                src_ref=src, dst_ref=dst, send_sem=send_sem.at[k, g, q], recv_sem=recv_sem.at[k, g, there],
                device_id=device(q), device_id_type=MESH))
        return copies

    def fill_sides(k, g, planes):
        base = k * groups * NPL + g * NPL
        for side, first in ((0, 0), (1, tile_w - BORDER)):
            for p in planes:
                for j in range(BORDER):
                    hsend[k, g, side, p * BORDER + j] = column(base + p, 0, first + j, tile_h)[...].astype(BF16)

    def send_early(k, g):
        copies = messages(k, g)
        fill_sides(k, g, range(2))
        for q in (8, 9):
            pl.when(exists(q))(copies[q].start)

    def send_late(k, g):
        base = k * groups * NPL + g * NPL
        copies = messages(k, g)
        fill_sides(k, g, range(2, NPL))
        for q in range(4, 8):
            dr, dc = steps[q]
            first = 0 if dc < 0 else tile_w - BORDER
            row = 0 if dr < 0 else tile_h - BORDER
            for p in range(NPL):
                for j in range(BORDER):
                    cstage[pl.ds((p * BORDER + j) * BORDER, BORDER)] = column(base + p, row, first + j, BORDER)[...]
            csend[k, g, q - 4] = cstage[...].astype(BF16)
        for q in (2, 3, 4, 5, 6, 7, 0, 1):
            pl.when(exists(q))(copies[q].start)

    def receive(k, g):
        base = k * groups * NPL + g * NPL
        for q in range(len(steps)):
            pl.when(exists(q))(_wait_recv(k, g, q))
        for q in (2, 3):
            first = -BORDER if q == 2 else tile_w

            @pl.when(exists(q))
            def _():
                for p in range(NPL):
                    for j in range(BORDER):
                        column(base + p, 0, first + j, tile_h)[...] = hrecv[k, g, q - 2, p * BORDER + j].astype(F32)
        for q in range(4, 8):
            dr, dc = steps[q]
            first = -BORDER if dc < 0 else tile_w
            row = -BORDER if dr < 0 else tile_h

            @pl.when(exists(q))
            def _():
                cstage[...] = crecv[k, g, q - 4].astype(F32)
                for p in range(NPL):
                    for j in range(BORDER):
                        column(base + p, row, first + j, BORDER)[...] = cstage[pl.ds((p * BORDER + j) * BORDER, BORDER)]

    def _wait_recv(k, g, q):
        base = k * groups * NPL + g * NPL
        dr, dc = steps[q]
        if dc == 0:
            land = 0 if dr < 0 else BORDER + tile_h
            dst = pad.at[pl.ds(base, NPL), pl.ds(land, BORDER), pl.ds(COL0, tile_w), :]
        elif dr == 0:
            dst = hrecv.at[k, g, q % 2, side_rows(q)]
        else:
            dst = crecv.at[k, g, q - 4]

        def wait():
            pltpu.make_async_remote_copy(
                src_ref=dst, dst_ref=dst, send_sem=send_sem.at[k, g, q], recv_sem=recv_sem.at[k, g, q],
                device_id=device(q), device_id_type=MESH).wait_recv()

        return wait

    def wait_send(k, g):
        copies = messages(k, g)
        for q in range(len(steps)):
            pl.when(exists(q))(copies[q].wait_send)

    def interior(plane):
        return pad.at[plane, pl.ds(BORDER, tile_h), pl.ds(COL0, tile_w), :]

    def rounded(values):
        return values.astype(BF16).astype(F32)

    def down_norm(g, i, slot):
        img = g * GI + i
        pltpu.make_async_copy(feat.at[img], fv.at[img], feat_sem.at[img]).wait()
        for w in range(in_w):
            x = fv[img, w].astype(F32)
            mean = jnp.sum(x, axis=0, keepdims=True) * (1.0 / ch_in)
            centered = x - mean
            var = jnp.sum(centered * centered, axis=0, keepdims=True) * (1.0 / ch_in)
            a = centered * lax.rsqrt(var + LN_EPS) * norm0[0, :, :in_h] + norm0[1, :, :in_h]
            ab[slot, pl.ds(w * ch_in, ch_in), :in_h] = a.astype(BF16)

    def down_conv(g, i, slot):
        turned = lax.dot_general(sel[...], ab[slot], (((1,), (1,)), ((), ())), preferred_element_type=F32).astype(BF16)
        pair = 2 * ch_in
        taps = []
        for w in range(tile_w):
            window = turned[:, w * pair:min(w * pair + 2 * LANES, turned.shape[1])]
            if window.shape[1] < 2 * LANES:
                window = jnp.concatenate([window, jnp.zeros((in_h, 2 * LANES - window.shape[1]), BF16)], axis=1)
            taps.append(jnp.concatenate([window[:tile_h], window[tile_h:]], axis=1))
        weights = jnp.concatenate([wd[...], wdt[i]], axis=1)
        d = jnp.dot(jnp.concatenate(taps, axis=0), weights, preferred_element_type=F32)
        head = rounded(d[:, :LANES] + vec[0, 0, 5:6])
        for w in range(tile_w):
            column(g * NPL + i, 0, w, tile_h)[...] = head[w * tile_h:(w + 1) * tile_h]
        ybuf[...] += d[:, LANES:]

    def down_group(g, _):
        @pl.when(g == 0)
        def _():
            for copy in weight_copies[4:]:
                copy.start()

        @pl.when(g < groups - 1)
        def _():
            for i in range(GI):
                img = (g + 1) * GI + i
                pltpu.make_async_copy(feat.at[img], fv.at[img], feat_sem.at[img]).start()

        ybuf[...] = jnp.zeros(ybuf.shape, F32)

        def two(j):
            down_norm(g, 2 * j, 0)
            down_norm(g, 2 * j + 1, 1)
            down_conv(g, 2 * j, 0)
            down_conv(g, 2 * j + 1, 1)

        two(0)

        @pl.when(g == 0)
        def _():
            count = jnp.int32(0)
            for q in range(8):
                count = count + exists(q).astype(jnp.int32)
            pl.semaphore_wait(barrier, count)

        send_early(0, g)
        two(1)
        tail = rounded(ybuf[...] + vec[0, 1, 5:6])
        for w in range(tile_w):
            column(g * NPL + GI, 0, w, tile_h)[...] = tail[w * tile_h:(w + 1) * tile_h]
        send_late(0, g)
        return 0

    half = tile_h // 2

    def taps_sum(k, part, plane, r0, count):
        accs = [None] * count
        for kw in range(7):
            xs = [pad[plane, r0 + i, COL0 - BORDER + kw:COL0 - BORDER + kw + 8, :] for i in range(count + 6)]
            for kh in range(7):
                w = jnp.broadcast_to(dwf[k, part, kh, kw:kw + 1, :], (8, LANES))
                for r in range(count):
                    term = xs[r + kh] * w
                    accs[r] = term if accs[r] is None else accs[r] + term
        return accs

    def depthwise(k, g):
        base = k * groups * NPL + g * NPL
        rows2 = (tile_h + 2) * tile_w

        def body(j, _):
            for strip in range(half // 12):
                r0 = j * half + strip * 12
                for r, acc in enumerate(taps_sum(k, 1, base + GI, r0, 12)):
                    ubuf[GI, pl.ds(pl.multiple_of((r0 + r) * 8, 8), 8)] = acc + vec[k, 1, 0:1]
            for strip in range(tile_h // 16):
                for r, acc in enumerate(taps_sum(k, 0, base + 2 + j, strip * 16, 16)):
                    ubuf[2 + j, pl.ds((strip * 16 + r) * 8, 8)] = acc + vec[k, 0, 0:1]

            parts = []
            for kw in range(0,7):
                shifted = pad[base + j, :, COL0 - BORDER + kw:COL0 - BORDER + kw + 8, :].astype(BF16).reshape(-1, LANES)
                for pair in range(4):
                    parts.append(shifted[pair * 16:pair * 16 + rows2])
            sums = jnp.dot(jnp.concatenate(parts, axis=1), diag[k, 0:3584], preferred_element_type=F32)
            part = sums[:pix, :LANES] + sums[8:pix + 8, LANES:]
            ubuf[j] = part + vec[k, 0, 0:1]
            return 0

        lax.fori_loop(0, 2, body, 0)

    LR = 64

    def norm(k):
        nw, nb = vec[k, 0, 1:2], vec[k, 0, 2:3]
        nwt, nbt = vec[k, 1, 1:2], vec[k, 1, 2:3]
        lane = lax.broadcasted_iota(jnp.int32, (LR, LANES), 1)
        channels = LANES + TAIL

        def body(t, _):
            rows = pl.ds(t * LR, LR)
            tail = ubuf[GI, rows]
            heads = [ubuf[i, rows] for i in range(GI)]
            own = [jnp.logical_and(lane >= i * TAIL, lane < (i + 1) * TAIL) for i in range(GI)]

            def pick(cols):
                res = cols[GI - 1]
                for i in range(GI - 2, -1, -1):
                    res = jnp.where(lane < (i + 1) * TAIL, cols[i], res)
                return res

            means = [jnp.sum(heads[i] + jnp.where(own[i], tail, 0.0), axis=-1, keepdims=True) * (1.0 / channels) for i in range(GI)]
            heads = [heads[i] - means[i] for i in range(GI)]
            tail = tail - pick(means)
            square = tail * tail
            rs = [lax.rsqrt(jnp.sum(heads[i] * heads[i] + jnp.where(own[i], square, 0.0), axis=-1, keepdims=True) * (1.0 / channels) + LN_EPS) for i in range(GI)]
            for i in range(GI):
                vbuf[i, rows] = (heads[i] * rs[i] * nw + nb).astype(BF16)
            vbuf[GI, rows] = (tail * pick(rs) * nwt + nbt).astype(BF16)
            return 0

        for t in range(pix // LR):
            body(t, 0)

    def mlp(k, g):
        base = k * groups * NPL + g * NPL
        nxt = groups * NPL + g * NPL
        b1 = pw1_b[k:k + 1, :].astype(F32) * HALF
        def up(i):
            v = jnp.concatenate([vbuf[i], vbuf[GI]], axis=1)
            return jnp.dot(v, jnp.concatenate([w1[k], w1t[k, i]], axis=0), preferred_element_type=F32)

        def act(x):
            x = x + b1
            return (x + x * lax.erf(x * RSQRT2X2)).astype(BF16)

        def down(i, hidden):
            y = lax.dot_general(hidden, jnp.concatenate([pw2[k, :LANES], w2t[k, i]], axis=0), (((1,), (1,)), ((), ())), preferred_element_type=F32)
            head = (y[:, :LANES] + vec[k, 0, 3:4]) * vec[k, 0, 4:5]
            new = interior(base + i)[...] + head.reshape(tile_h, tile_w, LANES)
            if k == 0:
                interior(nxt + i)[...] = rounded(new)
            else:
                obuf[g * GI + i, :, :, :LANES] = new.astype(BF16)
            return y[:, LANES:]

        x = up(0)
        for i in range(GI):
            hidden = act(x)
            if i < GI - 1:
                x = up(i + 1)
            tail = down(i, hidden)
            ybuf[...] = tail if i == 0 else ybuf[...] + tail
        tail = ((ybuf[...] + vec[k, 1, 3:4]) * vec[k, 1, 4:5]).reshape(tile_h, tile_w, LANES)
        new = interior(base + GI)[...] + tail
        if k == 0:
            interior(nxt + GI)[...] = rounded(new)
        else:
            for i in range(GI):
                obuf[g * GI + i, :, :, LANES:] = new[:, :, i * TAIL:(i + 1) * TAIL].astype(BF16)

    def out_copy(g):
        imgs = pl.ds(g * GI, GI)
        return pltpu.make_async_copy(obuf.at[imgs], out.at[imgs], out_sem.at[g])

    def block_group(k):
        def body(g, _):
            receive(k, g)
            depthwise(k, g)
            norm(k)
            mlp(k, g)
            if k == 0:
                send_early(1, g)
                send_late(1, g)
            else:
                out_copy(g).start()
            return 0
        return body

    lax.fori_loop(0, groups, down_group, 0)
    block_weights()
    lax.fori_loop(0, groups, block_group(0), 0)
    lax.fori_loop(0, groups, block_group(1), 0)

    def finish(g, _):
        wait_send(0, g)
        wait_send(1, g)
        out_copy(g).wait()
        return 0

    lax.fori_loop(0, groups, finish, 0)


def solution(mesh):
    rows_count = mesh.shape["sh"]
    cols_count = mesh.shape["sw"]
    act_spec = P("dp", "sh", "sw", None)

    def local_run(feat_map, norm0_w, norm0_b, down_w, down_b, dw_w, dw_b, norm_w, norm_b, pw1_w, pw1_b, pw2_w, pw2_b, layer_scale):
        images, in_h, in_w, ch_in = feat_map.shape
        tile_h, tile_w = in_h // 2, in_w // 2
        ch, hidden = pw1_w.shape[1:]
        groups = images // GI
        pix = tile_h * tile_w
        weights = [
            norm0_w.reshape(1, -1), norm0_b.reshape(1, -1), down_w, down_b, dw_w.transpose(1, 2, 0, 3), dw_b,
            norm_w, norm_b, pw1_w, pw1_b, pw2_w.transpose(0, 2, 1), pw2_b, layer_scale,
        ]
        hbm = pl.BlockSpec(memory_space=pl.ANY)
        return pl.pallas_call(
            functools.partial(kernel, rows_count, cols_count),
            out_shape=jax.ShapeDtypeStruct((images, tile_h, tile_w, ch), BF16),
            in_specs=[hbm] * (1 + len(weights)),
            out_specs=hbm,
            scratch_shapes=[pltpu.VMEM(w.shape, BF16) for w in weights] + [
                pltpu.VMEM((images, in_w, ch_in, in_h), BF16),
                pltpu.VMEM((2, in_w * ch_in, LANES), BF16),
                pltpu.VMEM((in_h, LANES), BF16),
                pltpu.VMEM((2, ch_in, LANES), F32),
                pltpu.VMEM((2 * groups * NPL, tile_h + 2 * BORDER + 2, ROW, LANES), F32),
                pltpu.VMEM((2, groups, 2, NPL * BORDER, tile_h, LANES), BF16),
                pltpu.VMEM((2, groups, 2, NPL * BORDER, tile_h, LANES), BF16),
                pltpu.VMEM((2, groups, 4, 48, LANES), BF16),
                pltpu.VMEM((2, groups, 4, 48, LANES), BF16),
                pltpu.VMEM((48, LANES), F32),
                pltpu.VMEM((NPL, pix, LANES), F32),
                pltpu.VMEM((NPL, pix, LANES), BF16),
                pltpu.VMEM((pix, LANES), F32),
                pltpu.VMEM((4 * LANES, LANES), BF16),
                pltpu.VMEM((GI, 4 * LANES, LANES), BF16),
                pltpu.VMEM((2, LANES, hidden), BF16),
                pltpu.VMEM((2, GI, LANES, hidden), BF16),
                pltpu.VMEM((2, GI, LANES, hidden), BF16),
                pltpu.VMEM((2, 2, 7, 8, LANES), F32),
                pltpu.VMEM((LANES, LANES), BF16),
                pltpu.VMEM((2, 7 * 4 * LANES, 2 * LANES), BF16),
                pltpu.VMEM((2, 2, 8, LANES), F32),
                pltpu.VMEM((images, tile_h, tile_w, ch), BF16),
                pltpu.SemaphoreType.DMA((images,)),
                pltpu.SemaphoreType.DMA((len(weights),)),
                pltpu.SemaphoreType.DMA((groups,)),
                pltpu.SemaphoreType.DMA((2, groups, 10)),
                pltpu.SemaphoreType.DMA((2, groups, 10)),
            ],
            compiler_params=pltpu.CompilerParams(collective_id=0, has_side_effects=True, vmem_limit_bytes=63 * 1024 * 1024),
        )(feat_map.transpose(0, 2, 3, 1), *weights)

    return jax.shard_map(local_run, mesh=mesh, in_specs=(act_spec,) + (P(),) * 13, out_specs=act_spec, check_vma=False)
```

```python
import functools

import jax
import jax.numpy as jnp
from jax import lax
from jax.experimental import pallas as pl
from jax.experimental.pallas import tpu as pltpu
from jax.sharding import PartitionSpec as P

LN_EPS = 1e-6
MESH = pl.DeviceIdType.MESH
GI = 4
NPL = GI + 1
LANES = 128
TAIL = 32
ROW = 24
COL0 = 8
BORDER = 3
HALF = 0.5
RSQRT2X2 = 1.4142135623730951

F32 = jnp.float32
BF16 = jnp.bfloat16


def kernel(
    rows_count, cols_count,
    feat, norm0_w_hbm, norm0_b_hbm, down_w_hbm, down_b_hbm, dw_w_hbm, dw_b_hbm, norm_w_hbm, norm_b_hbm, pw1_w_hbm, pw1_b_hbm, pw2_w_hbm, pw2_b_hbm, scale_hbm,
    out,
    norm0_w, norm0_b, down_w, down_b, dw_w, dw_b, norm_w, norm_b, pw1, pw1_b, pw2, pw2_b, layer_scale,
    fv, ab, sel, norm0, pad, hsend, hrecv, csend, crecv, cstage, ubuf, vbuf, ybuf, wd, wdt, w1, w1t, w2t, dwf, eye, diag, vec, obuf,
    feat_sem, weight_sem, out_sem, send_sem, recv_sem,
):
    images, in_w, ch_in, in_h = fv.shape
    groups = images // GI
    tile_h, tile_w = obuf.shape[1], obuf.shape[2]
    pix = tile_h * tile_w
    my_row, my_col = lax.axis_index("sh"), lax.axis_index("sw")
    has_up, has_down = my_row > 0, my_row < rows_count - 1
    has_left, has_right = my_col > 0, my_col < cols_count - 1

    steps = [(-1, 0), (1, 0), (0, -1), (0, 1), (-1, -1), (-1, 1), (1, -1), (1, 1)]
    steps += [(0, -1), (0, 1)]
    row_ok = {-1: has_up, 0: None, 1: has_down}
    col_ok = {-1: has_left, 0: None, 1: has_right}

    def exists(q):
        dr, dc = steps[q]
        if row_ok[dr] is None:
            return col_ok[dc]
        if col_ok[dc] is None:
            return row_ok[dr]
        return jnp.logical_and(row_ok[dr], col_ok[dc])

    def opposite(q):
        dr, dc = steps[q]
        return q ^ 1 if dr == 0 else steps.index((-dr, -dc))

    def device(q):
        dr, dc = steps[q]
        return {"sh": my_row + dr, "sw": my_col + dc}

    feat_copies = [pltpu.make_async_copy(feat.at[i], fv.at[i], feat_sem.at[i]) for i in range(images)]
    weights_hbm = [norm0_w_hbm, norm0_b_hbm, down_w_hbm, down_b_hbm, dw_w_hbm, dw_b_hbm, norm_w_hbm, norm_b_hbm, pw1_w_hbm, pw1_b_hbm, pw2_w_hbm, pw2_b_hbm, scale_hbm]
    weights_here = [norm0_w, norm0_b, down_w, down_b, dw_w, dw_b, norm_w, norm_b, pw1, pw1_b, pw2, pw2_b, layer_scale]
    weight_copies = [pltpu.make_async_copy(far, near, weight_sem.at[n]) for n, (far, near) in enumerate(zip(weights_hbm, weights_here))]
    for copy in weight_copies[:4] + feat_copies[:GI]:
        copy.start()

    barrier = pltpu.get_barrier_semaphore()
    for q in range(8):
        @pl.when(exists(q))
        def _():
            pl.semaphore_signal(barrier, inc=1, device_id=device(q), device_id_type=MESH)

    def zero_rows(first):
        def body(p, _):
            pad[p, pl.ds(first, BORDER)] = jnp.zeros((BORDER, ROW, LANES), F32)
            return 0
        lax.fori_loop(0, pad.shape[0], body, 0)

    def zero_cols(first):
        def body(p, _):
            pad[p, :, pl.ds(first, 8)] = jnp.zeros((pad.shape[1], 8, LANES), F32)
            return 0
        lax.fori_loop(0, pad.shape[0], body, 0)

    pl.when(jnp.logical_not(has_up))(lambda: zero_rows(0))
    pl.when(jnp.logical_not(has_down))(lambda: zero_rows(BORDER + tile_h))
    pl.when(jnp.logical_not(has_left))(lambda: zero_cols(0))
    pl.when(jnp.logical_not(has_right))(lambda: zero_cols(COL0 + tile_w))

    ab[...] = jnp.zeros(ab.shape, BF16)
    row_id = lax.broadcasted_iota(jnp.int32, sel.shape, 0)
    col_id = lax.broadcasted_iota(jnp.int32, sel.shape, 1)
    picked = jnp.where(row_id < tile_h, 2 * row_id, 2 * (row_id - tile_h) + 1)
    sel[...] = jnp.where(col_id == picked, 1.0, 0.0).astype(BF16)
    for copy in weight_copies[:4]:
        copy.wait()
    norm0[0] = jnp.broadcast_to(norm0_w[...].astype(F32), (LANES, ch_in)).T
    norm0[1] = jnp.broadcast_to(norm0_b[...].astype(F32), (LANES, ch_in)).T
    cstage[...] = jnp.zeros(cstage.shape, F32)

    def tail_at(tail, slot):
        rows = tail.shape[0]
        parts = [tail]
        if slot:
            parts = [jnp.zeros((rows, TAIL * slot), tail.dtype)] + parts
        if slot < GI - 1:
            parts = parts + [jnp.zeros((rows, TAIL * (GI - 1 - slot)), tail.dtype)]
        return jnp.concatenate(parts, axis=1)

    for kh in range(2):
        zeros = jnp.zeros((2 * LANES - 2 * ch_in, LANES), BF16)
        wd[pl.ds(kh * 2 * LANES + 2 * ch_in, 2 * LANES - 2 * ch_in)] = zeros
        for kw in range(2):
            taps = down_w[kh, kw].astype(F32)
            rows = pl.ds(kh * 2 * LANES + kw * ch_in, ch_in)
            wd[rows] = taps[:, :LANES].astype(BF16)
            for slot in range(GI):
                wdt[slot, rows] = tail_at(taps[:, LANES:], slot).astype(BF16)
        for slot in range(GI):
            wdt[slot, pl.ds(kh * 2 * LANES + 2 * ch_in, 2 * LANES - 2 * ch_in)] = zeros

    def block_weights():
        for copy in weight_copies[4:]:
            copy.wait()
        for kh in range(7):
            for kw in range(7):
                taps = dw_w[kh, kw].astype(F32)
                tails = jnp.concatenate([taps[:, LANES:]] * GI, axis=1)
                for k in range(2):
                    dwf[k, 0, kh, kw:kw + 1] = taps[k:k + 1, :LANES]
                    dwf[k, 1, kh, kw:kw + 1] = tails[k:k + 1]
        names = [dw_b, norm_w, norm_b, pw2_b, layer_scale]
        for k in range(2):
            for j, ref in enumerate(names):
                head, tail = split(ref[k:k + 1, :])
                vec[k, 0, j:j + 1] = head
                vec[k, 1, j:j + 1] = tail
        for k in range(2):
            w1[k] = (pw1[k, :LANES].astype(F32) * HALF).astype(BF16)
            up_tail = (pw1[k, LANES:].astype(F32) * HALF).astype(BF16)
            for slot in range(GI):
                for other in range(GI):
                    rows = pl.ds(TAIL * other, TAIL)
                    w1t[k, slot, rows] = up_tail if other == slot else jnp.zeros(up_tail.shape, BF16)
                    w2t[k, slot, rows] = pw2[k, LANES:] if other == slot else jnp.zeros(up_tail.shape, BF16)
        for kw in range(7):
            spread(kw, 0)

    eye[...] = jnp.where(lax.broadcasted_iota(jnp.int32, eye.shape, 0) == lax.broadcasted_iota(jnp.int32, eye.shape, 1), 1.0, 0.0).astype(BF16)

    def spread(kw, _):
        unit = eye[...]
        for k in range(2):
            for kh in range(8):
                if kh < 7:
                    tap = jnp.broadcast_to(dwf[k, 0, kh, kw:kw + 1], (16, LANES)).astype(BF16)
                    block = unit * jnp.concatenate([tap] * (LANES // 16), axis=0)
                else:
                    block = jnp.zeros((LANES, LANES), BF16)
                diag[k, pl.ds((kw * 4 + kh // 2) * LANES, LANES), kh % 2 * LANES:(kh % 2 + 1) * LANES] = block
        return 0

    pad[:, tile_h + 2 * BORDER:] = jnp.zeros((pad.shape[0], 2, ROW, LANES), F32)

    def split(row):
        row = row.astype(F32)
        return row[:, :LANES], jnp.concatenate([row[:, LANES:]] * GI, axis=1)

    head, tail = split(down_b[...].reshape(1, -1))
    vec[0, 0, 5:6] = head
    vec[0, 1, 5:6] = tail

    flat = pad.reshape(pad.shape[0], pad.shape[1] * ROW, LANES)

    def column(plane, row, col, count):
        return flat.at[plane, pl.ds((BORDER + row) * ROW + COL0 + col, count, stride=ROW), :]

    def side_rows(q):
        return pl.ds(0, 2 * BORDER) if q >= 8 else pl.ds(2 * BORDER, (NPL - 2) * BORDER)

    def messages(k, g):
        base = k * groups * NPL + g * NPL
        planes = pl.ds(base, NPL)
        copies = []
        for q, (dr, dc) in enumerate(steps):
            there = opposite(q)
            if dc == 0:
                first = BORDER if dr < 0 else tile_h
                land = BORDER + tile_h if dr < 0 else 0
                src = pad.at[planes, pl.ds(first, BORDER), pl.ds(COL0, tile_w), :]
                dst = pad.at[planes, pl.ds(land, BORDER), pl.ds(COL0, tile_w), :]
            elif dr == 0:
                src = hsend.at[k, g, q % 2, side_rows(q)]
                dst = hrecv.at[k, g, there % 2, side_rows(q)]
            else:
                src = csend.at[k, g, q - 4]
                dst = crecv.at[k, g, there - 4]
            copies.append(pltpu.make_async_remote_copy(
                src_ref=src, dst_ref=dst, send_sem=send_sem.at[k, g, q], recv_sem=recv_sem.at[k, g, there],
                device_id=device(q), device_id_type=MESH))
        return copies

    def fill_sides(k, g, planes):
        base = k * groups * NPL + g * NPL
        for side, first in ((0, 0), (1, tile_w - BORDER)):
            for p in planes:
                for j in range(BORDER):
                    hsend[k, g, side, p * BORDER + j] = column(base + p, 0, first + j, tile_h)[...].astype(BF16)

    def send_early(k, g):
        copies = messages(k, g)
        fill_sides(k, g, range(2))
        for q in (8, 9):
            pl.when(exists(q))(copies[q].start)

    def send_late(k, g):
        base = k * groups * NPL + g * NPL
        copies = messages(k, g)
        fill_sides(k, g, range(2, NPL))
        for q in range(4, 8):
            dr, dc = steps[q]
            first = 0 if dc < 0 else tile_w - BORDER
            row = 0 if dr < 0 else tile_h - BORDER
            for p in range(NPL):
                for j in range(BORDER):
                    cstage[pl.ds((p * BORDER + j) * BORDER, BORDER)] = column(base + p, row, first + j, BORDER)[...]
            csend[k, g, q - 4] = cstage[...].astype(BF16)
        for q in (2, 3, 4, 5, 6, 7, 0, 1):
            pl.when(exists(q))(copies[q].start)

    def receive(k, g):
        base = k * groups * NPL + g * NPL
        for q in range(len(steps)):
            pl.when(exists(q))(_wait_recv(k, g, q))
        for q in (2, 3):
            first = -BORDER if q == 2 else tile_w

            @pl.when(exists(q))
            def _():
                for p in range(NPL):
                    for j in range(BORDER):
                        column(base + p, 0, first + j, tile_h)[...] = hrecv[k, g, q - 2, p * BORDER + j].astype(F32)
        for q in range(4, 8):
            dr, dc = steps[q]
            first = -BORDER if dc < 0 else tile_w
            row = -BORDER if dr < 0 else tile_h

            @pl.when(exists(q))
            def _():
                cstage[...] = crecv[k, g, q - 4].astype(F32)
                for p in range(NPL):
                    for j in range(BORDER):
                        column(base + p, row, first + j, BORDER)[...] = cstage[pl.ds((p * BORDER + j) * BORDER, BORDER)]

    def _wait_recv(k, g, q):
        base = k * groups * NPL + g * NPL
        dr, dc = steps[q]
        if dc == 0:
            land = 0 if dr < 0 else BORDER + tile_h
            dst = pad.at[pl.ds(base, NPL), pl.ds(land, BORDER), pl.ds(COL0, tile_w), :]
        elif dr == 0:
            dst = hrecv.at[k, g, q % 2, side_rows(q)]
        else:
            dst = crecv.at[k, g, q - 4]

        def wait():
            pltpu.make_async_remote_copy(
                src_ref=dst, dst_ref=dst, send_sem=send_sem.at[k, g, q], recv_sem=recv_sem.at[k, g, q],
                device_id=device(q), device_id_type=MESH).wait_recv()

        return wait

    def wait_send(k, g):
        copies = messages(k, g)
        for q in range(len(steps)):
            pl.when(exists(q))(copies[q].wait_send)

    def interior(plane):
        return pad.at[plane, pl.ds(BORDER, tile_h), pl.ds(COL0, tile_w), :]

    def rounded(values):
        return values.astype(BF16).astype(F32)

    def down_norm(g, i, slot):
        img = g * GI + i
        pltpu.make_async_copy(feat.at[img], fv.at[img], feat_sem.at[img]).wait()
        for w in range(in_w):
            x = fv[img, w].astype(F32)
            mean = jnp.sum(x, axis=0, keepdims=True) * (1.0 / ch_in)
            centered = x - mean
            var = jnp.sum(centered * centered, axis=0, keepdims=True) * (1.0 / ch_in)
            a = centered * lax.rsqrt(var + LN_EPS) * norm0[0, :, :in_h] + norm0[1, :, :in_h]
            ab[slot, pl.ds(w * ch_in, ch_in), :in_h] = a.astype(BF16)

    def down_conv(g, i, slot):
        turned = lax.dot_general(sel[...], ab[slot], (((1,), (1,)), ((), ())), preferred_element_type=F32).astype(BF16)
        pair = 2 * ch_in
        taps = []
        for w in range(tile_w):
            window = turned[:, w * pair:min(w * pair + 2 * LANES, turned.shape[1])]
            if window.shape[1] < 2 * LANES:
                window = jnp.concatenate([window, jnp.zeros((in_h, 2 * LANES - window.shape[1]), BF16)], axis=1)
            taps.append(jnp.concatenate([window[:tile_h], window[tile_h:]], axis=1))
        weights = jnp.concatenate([wd[...], wdt[i]], axis=1)
        d = jnp.dot(jnp.concatenate(taps, axis=0), weights, preferred_element_type=F32)
        head = rounded(d[:, :LANES] + vec[0, 0, 5:6])
        for w in range(tile_w):
            column(g * NPL + i, 0, w, tile_h)[...] = head[w * tile_h:(w + 1) * tile_h]
        ybuf[...] += d[:, LANES:]

    def down_group(g, _):
        @pl.when(g == 0)
        def _():
            for copy in weight_copies[4:]:
                copy.start()

        @pl.when(g < groups - 1)
        def _():
            for i in range(GI):
                img = (g + 1) * GI + i
                pltpu.make_async_copy(feat.at[img], fv.at[img], feat_sem.at[img]).start()

        ybuf[...] = jnp.zeros(ybuf.shape, F32)

        def two(j):
            down_norm(g, 2 * j, 0)
            down_norm(g, 2 * j + 1, 1)
            down_conv(g, 2 * j, 0)
            down_conv(g, 2 * j + 1, 1)

        two(0)

        @pl.when(g == 0)
        def _():
            count = jnp.int32(0)
            for q in range(8):
                count = count + exists(q).astype(jnp.int32)
            pl.semaphore_wait(barrier, count)

        send_early(0, g)
        two(1)
        tail = rounded(ybuf[...] + vec[0, 1, 5:6])
        for w in range(tile_w):
            column(g * NPL + GI, 0, w, tile_h)[...] = tail[w * tile_h:(w + 1) * tile_h]
        send_late(0, g)
        return 0

    half = tile_h // 2

    def taps_sum(k, part, plane, r0, count):
        start = jnp.broadcast_to(vec[k, part, 0:1], (8, LANES))
        accs = [start] * count
        for kw in range(7):
            xs = [pad[plane, r0 + i, COL0 - BORDER + kw:COL0 - BORDER + kw + 8, :] for i in range(count + 6)]
            for kh in range(7):
                w = jnp.broadcast_to(dwf[k, part, kh, kw:kw + 1, :], (8, LANES))
                for r in range(count):
                    term = xs[r + kh] * w
                    accs[r] = accs[r] + term
        return accs

    def depthwise(k, g):
        base = k * groups * NPL + g * NPL
        rows2 = (tile_h + 2) * tile_w

        def body(j, _):
            for strip in range(half // 12):
                r0 = j * half + strip * 12
                for r, acc in enumerate(taps_sum(k, 1, base + GI, r0, 12)):
                    ubuf[GI, pl.ds(pl.multiple_of((r0 + r) * 8, 8), 8)] = acc
            for strip in range(tile_h // 16):
                for r, acc in enumerate(taps_sum(k, 0, base + 2 + j, strip * 16, 16)):
                    ubuf[2 + j, pl.ds((strip * 16 + r) * 8, 8)] = acc

            parts = []
            for kw in range(0,7):
                shifted = pad[base + j, :, COL0 - BORDER + kw:COL0 - BORDER + kw + 8, :].astype(BF16).reshape(-1, LANES)
                for pair in range(4):
                    parts.append(shifted[pair * 16:pair * 16 + rows2])
            sums = jnp.dot(jnp.concatenate(parts, axis=1), diag[k, 0:3584], preferred_element_type=F32)
            part = sums[:pix, :LANES] + sums[8:pix + 8, LANES:]
            ubuf[j] = part + vec[k, 0, 0:1]
            return 0

        lax.fori_loop(0, 2, body, 0)

    LR = 64

    def norm(k):
        nw, nb = vec[k, 0, 1:2], vec[k, 0, 2:3]
        nwt, nbt = vec[k, 1, 1:2], vec[k, 1, 2:3]
        lane = lax.broadcasted_iota(jnp.int32, (LR, LANES), 1)
        channels = LANES + TAIL

        def body(t, _):
            rows = pl.ds(t * LR, LR)
            tail = ubuf[GI, rows]
            heads = [ubuf[i, rows] for i in range(GI)]
            own = [jnp.logical_and(lane >= i * TAIL, lane < (i + 1) * TAIL) for i in range(GI)]

            def pick(cols):
                res = cols[GI - 1]
                for i in range(GI - 2, -1, -1):
                    res = jnp.where(lane < (i + 1) * TAIL, cols[i], res)
                return res

            means = [jnp.sum(heads[i] + jnp.where(own[i], tail, 0.0), axis=-1, keepdims=True) * (1.0 / channels) for i in range(GI)]
            heads = [heads[i] - means[i] for i in range(GI)]
            tail = tail - pick(means)
            square = tail * tail
            rs = [lax.rsqrt(jnp.sum(heads[i] * heads[i] + jnp.where(own[i], square, 0.0), axis=-1, keepdims=True) * (1.0 / channels) + LN_EPS) for i in range(GI)]
            for i in range(GI):
                vbuf[i, rows] = (heads[i] * rs[i] * nw + nb).astype(BF16)
            vbuf[GI, rows] = (tail * pick(rs) * nwt + nbt).astype(BF16)
            return 0

        for t in range(pix // LR):
            body(t, 0)

    def mlp(k, g):
        base = k * groups * NPL + g * NPL
        nxt = groups * NPL + g * NPL
        b1 = pw1_b[k:k + 1, :].astype(F32) * HALF
        def up(i):
            v = jnp.concatenate([vbuf[i], vbuf[GI]], axis=1)
            return jnp.dot(v, jnp.concatenate([w1[k], w1t[k, i]], axis=0), preferred_element_type=F32)

        def act(x):
            x = x + b1
            return (x + x * lax.erf(x * RSQRT2X2)).astype(BF16)

        def down(i, hidden):
            y = lax.dot_general(hidden, jnp.concatenate([pw2[k, :LANES], w2t[k, i]], axis=0), (((1,), (1,)), ((), ())), preferred_element_type=F32)
            head = (y[:, :LANES] + vec[k, 0, 3:4]) * vec[k, 0, 4:5]
            new = interior(base + i)[...] + head.reshape(tile_h, tile_w, LANES)
            if k == 0:
                interior(nxt + i)[...] = rounded(new)
            else:
                obuf[g * GI + i, :, :, :LANES] = new.astype(BF16)
            return y[:, LANES:]

        x = up(0)
        for i in range(GI):
            hidden = act(x)
            if i < GI - 1:
                x = up(i + 1)
            tail = down(i, hidden)
            ybuf[...] = tail if i == 0 else ybuf[...] + tail
        tail = ((ybuf[...] + vec[k, 1, 3:4]) * vec[k, 1, 4:5]).reshape(tile_h, tile_w, LANES)
        new = interior(base + GI)[...] + tail
        if k == 0:
            interior(nxt + GI)[...] = rounded(new)
        else:
            for i in range(GI):
                obuf[g * GI + i, :, :, LANES:] = new[:, :, i * TAIL:(i + 1) * TAIL].astype(BF16)

    def out_copy(g):
        imgs = pl.ds(g * GI, GI)
        return pltpu.make_async_copy(obuf.at[imgs], out.at[imgs], out_sem.at[g])

    def block_group(k):
        def body(g, _):
            receive(k, g)
            depthwise(k, g)
            norm(k)
            mlp(k, g)
            if k == 0:
                send_early(1, g)
                send_late(1, g)
            else:
                out_copy(g).start()
            return 0
        return body

    lax.fori_loop(0, groups, down_group, 0)
    block_weights()
    lax.fori_loop(0, groups, block_group(0), 0)
    lax.fori_loop(0, groups, block_group(1), 0)

    def finish(g, _):
        wait_send(0, g)
        wait_send(1, g)
        out_copy(g).wait()
        return 0

    lax.fori_loop(0, groups, finish, 0)


def solution(mesh):
    rows_count = mesh.shape["sh"]
    cols_count = mesh.shape["sw"]
    act_spec = P("dp", "sh", "sw", None)

    def local_run(feat_map, norm0_w, norm0_b, down_w, down_b, dw_w, dw_b, norm_w, norm_b, pw1_w, pw1_b, pw2_w, pw2_b, layer_scale):
        images, in_h, in_w, ch_in = feat_map.shape
        tile_h, tile_w = in_h // 2, in_w // 2
        ch, hidden = pw1_w.shape[1:]
        groups = images // GI
        pix = tile_h * tile_w
        weights = [
            norm0_w.reshape(1, -1), norm0_b.reshape(1, -1), down_w, down_b, dw_w.transpose(1, 2, 0, 3), dw_b,
            norm_w, norm_b, pw1_w, pw1_b, pw2_w.transpose(0, 2, 1), pw2_b, layer_scale,
        ]
        hbm = pl.BlockSpec(memory_space=pl.ANY)
        return pl.pallas_call(
            functools.partial(kernel, rows_count, cols_count),
            out_shape=jax.ShapeDtypeStruct((images, tile_h, tile_w, ch), BF16),
            in_specs=[hbm] * (1 + len(weights)),
            out_specs=hbm,
            scratch_shapes=[pltpu.VMEM(w.shape, BF16) for w in weights] + [
                pltpu.VMEM((images, in_w, ch_in, in_h), BF16),
                pltpu.VMEM((2, in_w * ch_in, LANES), BF16),
                pltpu.VMEM((in_h, LANES), BF16),
                pltpu.VMEM((2, ch_in, LANES), F32),
                pltpu.VMEM((2 * groups * NPL, tile_h + 2 * BORDER + 2, ROW, LANES), F32),
                pltpu.VMEM((2, groups, 2, NPL * BORDER, tile_h, LANES), BF16),
                pltpu.VMEM((2, groups, 2, NPL * BORDER, tile_h, LANES), BF16),
                pltpu.VMEM((2, groups, 4, 48, LANES), BF16),
                pltpu.VMEM((2, groups, 4, 48, LANES), BF16),
                pltpu.VMEM((48, LANES), F32),
                pltpu.VMEM((NPL, pix, LANES), F32),
                pltpu.VMEM((NPL, pix, LANES), BF16),
                pltpu.VMEM((pix, LANES), F32),
                pltpu.VMEM((4 * LANES, LANES), BF16),
                pltpu.VMEM((GI, 4 * LANES, LANES), BF16),
                pltpu.VMEM((2, LANES, hidden), BF16),
                pltpu.VMEM((2, GI, LANES, hidden), BF16),
                pltpu.VMEM((2, GI, LANES, hidden), BF16),
                pltpu.VMEM((2, 2, 7, 8, LANES), F32),
                pltpu.VMEM((LANES, LANES), BF16),
                pltpu.VMEM((2, 7 * 4 * LANES, 2 * LANES), BF16),
                pltpu.VMEM((2, 2, 8, LANES), F32),
                pltpu.VMEM((images, tile_h, tile_w, ch), BF16),
                pltpu.SemaphoreType.DMA((images,)),
                pltpu.SemaphoreType.DMA((len(weights),)),
                pltpu.SemaphoreType.DMA((groups,)),
                pltpu.SemaphoreType.DMA((2, groups, 10)),
                pltpu.SemaphoreType.DMA((2, groups, 10)),
            ],
            compiler_params=pltpu.CompilerParams(collective_id=0, has_side_effects=True, vmem_limit_bytes=63 * 1024 * 1024),
        )(feat_map.transpose(0, 2, 3, 1), *weights)

    return jax.shard_map(local_run, mesh=mesh, in_specs=(act_spec,) + (P(),) * 13, out_specs=act_spec, check_vma=False)
```
